32 devices in a mesh: gx: 2 (over y), gy: 4 (over z), gz: 4 (over x, core).
Axes of the slice: x: 2, y: 2, z: 4, core: 2. Of those that a mesh axis runs over, the one named last changes fastest.
Arguments:
- velocity: float32 [8192, 3, 128], P(('gx', 'gy', 'gz')), may hold values from -6 to 6
- cell_index: int32 [8192, 128], P(('gx', 'gy', 'gz')), may hold values from 0 to 5804
- block_target: int32 [8192, 1], P(('gx', 'gy', 'gz')), may hold values from 0 to 31; in each aligned block of 256 rows (0 to 255, 256 to 511, ...) at most 12 rows name the same one
- rotation_axis: int32 [32, 32, 32], replicated, may hold values from 0 to 63
- grid_shift: int32 [3], replicated, may hold values from 0 to 31
Outputs:
- brick_velocity: float32 [32, 32, 12, 3, 128], P(('gx', 'gy', 'gz'))
- cell_flow: float32 [3, 8, 32, 512], P(None, 'gx', 'gy', 'gz')
The draws below stay inside these ranges and needn't reach their ends.
Inputs may be any that keep to these rules, and one draw needn't show every extreme that they name: `block_target`: among the blocks that one device holds, no brick is named by more than 12 blocks, a bound that some block reaches.
All inputs are finite; a program needn't handle non-finite values.
Results may differ from the reference program's by a relative error of at most 0.0003.
Values sent between devices are 32-bit elements; how exact they have to be, the bound alone decides.
A program may use at most 64 MiB of HBM per device.

```python
import math
import jax
import jax.numpy as jnp
import numpy as np
from jax import lax

CX = 4
CY = 8
CZ = 128
BLK_DEV = 256
BROWS = 128
NAX = 64
APER = 32
MOST = 12
NBLK = 8192
NCX = 8
NCY = 32
NCZ = 512
N_GY = 4
N_GZ = 4
DEVICES = 32


def with_ends(entries, rng, least, largest):
    spot = [jax.random.randint(jax.random.fold_in(rng, axis), (), 0, length) for axis, length in enumerate(entries.shape)]
    main_axis = entries.shape.index(max(entries.shape))
    neighbour = spot[:main_axis] + [(spot[main_axis] + 1) % entries.shape[main_axis]] + spot[main_axis + 1:]
    return entries.at[tuple(spot)].set(least).at[tuple(neighbour)].set(largest)


def shard_levels(stream_key, extent, cuts, least, high):
    factor_of = 1.0
    for axis_at, parts in cuts:
        draws = jax.random.uniform(jax.random.fold_in(jax.random.fold_in(stream_key, 6), axis_at), (parts,), jnp.float32, least / len(cuts), high / len(cuts))
        factor_of = factor_of * jnp.repeat(jnp.exp(draws), extent[axis_at] // parts).reshape((-1,) + (1,) * (len(extent) - 1 - axis_at))
    return factor_of


def routed_block(key, own, number, rows, amount, top, limit, slope):
    sequence = jax.random.permutation(key, amount)
    packed, common = load_shares(amount, rows * top, limit, slope, True), load_shares(amount, rows * top, limit, slope, False)
    places = jnp.arange(amount)

    def named(tallies, rotation):
        used = int((tallies > 0).sum())
        fixed = max(1, used // 4)
        moved = fixed + (places - fixed + rotation * (used - fixed)) % max(1, amount - fixed)
        return jnp.zeros((amount,), jnp.int32).at[sequence[jnp.where(places < fixed, places, moved)]].set(jnp.asarray(tallies, jnp.int32))

    tallies = jnp.where(number % 4 == 0, named(packed, number // 4), named(common, number - number // 4 - 1))
    mixed = jax.random.permutation(jax.random.fold_in(own, 3), amount)
    source_of, sink = mixed[0:amount // 2 * 2:2], mixed[1:amount // 2 * 2:2]
    room = jnp.minimum(tallies[source_of] - 1, limit - tallies[sink]) // 2
    room = jnp.where((source_of == sequence[0]) | (sink == sequence[0]) | (tallies[sink] == 0), 0, jnp.maximum(room, 0))
    moved = jax.random.randint(jax.random.fold_in(own, 4), (amount // 2,), 0, 1 << 20) % (room + 1)
    tallies = tallies.at[source_of].add(-moved).at[sink].add(moved)
    members = jnp.searchsorted(jnp.cumsum(tallies), jnp.arange(rows * top), side="right").astype(jnp.int32)
    table = members.reshape(top, rows).T
    table = table[jax.random.permutation(jax.random.fold_in(own, 1), rows)]
    rotation = jax.random.randint(jax.random.fold_in(own, 2), (rows, 1), 0, top)
    return jnp.take_along_axis(table, (jnp.arange(top)[None, :] + rotation) % top, axis=1)


def load_shares(amount, total, most, skew, full):
    portions = [(1 << 20) // math.isqrt(grade ** skew) + 1 for grade in range(1, amount + 1)]
    largest = most if full else min(most, max(-(-total // amount), total * portions[0] // sum(portions)))
    least = 1 if total - largest >= amount - 1 else 0
    given, surplus = [largest] + [least] * (amount - 1), total - largest - least * (amount - 1)
    while surplus > 0:
        movable = [i for i in range(1, amount) if given[i] < largest] or [i for i in range(1, amount) if given[i] < most]
        mass, left = sum([portions[i] for i in movable]), surplus
        for i in movable:
            addition = min(most - given[i], max(1, left * portions[i] // mass), surplus)
            given[i] = given[i] + addition
            surplus = surplus - addition
    return np.array(given)


def normal_values(key, dims, spread, limit, split=(), kind=jnp.bfloat16):
    values = spread * jax.random.normal(key, dims, jnp.float32)
    if split:
        values = values * shard_levels(key, dims, split, -0.22, 0.18)
    return jnp.clip(values, -limit, limit).astype(kind)


def setup_inputs(seed: int = 0) -> dict:
    splits = jax.random.split(jax.random.key(seed), 6)
    velocity = normal_values(splits[0], (NBLK, 3, BROWS), 1.0, 6.0, ((0, 32),), jnp.float32)
    cell_index = with_ends(jax.random.randint(splits[1], (NBLK, BROWS), 0, (CX + 1) * (CY + 1) * (CZ + 1)), jax.random.fold_in(splits[1], 1), 0, ((CX + 1) * (CY + 1) * (CZ + 1)) - 1).astype(jnp.int32)
    block_target_keys = jax.random.split(jax.random.fold_in(splits[2], 1), NBLK // BLK_DEV)
    block_target_turns = jax.random.permutation(jax.random.fold_in(splits[2], 3), NBLK // BLK_DEV)
    block_target = jax.vmap(lambda own, number: routed_block(jax.random.fold_in(splits[2], 2), own, number, BLK_DEV, DEVICES, 1, MOST, 1))(block_target_keys, block_target_turns).reshape((NBLK, 1))
    rotation_axis = with_ends(jax.random.randint(splits[3], (APER, APER, APER), 0, NAX), jax.random.fold_in(splits[3], 1), 0, NAX - 1).astype(jnp.int32)
    grid_shift = jax.random.randint(splits[4], (3,), 0, APER).astype(jnp.int32)
    return dict(velocity=velocity, cell_index=cell_index, block_target=block_target, rotation_axis=rotation_axis, grid_shift=grid_shift)


angle_cosine = -0.6427876096865393
angle_sine = 0.766044443118978

def axis_table():
    counter = jnp.arange(NAX, dtype=jnp.float32) + 0.5
    height = 1.0 - 2.0 * counter / NAX
    radius = jnp.sqrt(jnp.maximum(1.0 - height * height, 0.0))
    turning = counter * 2.399963229728653
    return jnp.stack([radius * jnp.cos(turning), radius * jnp.sin(turning), height])

def rotate_about(direction, relative):
    inner_product = direction[0] * relative[0] + direction[1] * relative[1] + direction[2] * relative[2]
    crossed = [direction[1] * relative[2] - direction[2] * relative[1], direction[2] * relative[0] - direction[0] * relative[2], direction[0] * relative[1] - direction[1] * relative[0]]
    return [relative[component] * angle_cosine + crossed[component] * angle_sine + direction[component] * inner_product * (1.0 - angle_cosine) for component in range(3)]

def reference(velocity, cell_index, block_target, rotation_axis, grid_shift):
    blocks = velocity.shape[0]
    devices = blocks // BLK_DEV
    target = block_target[:, 0]

    def ranks_of(targets):
        onehot = (targets[:, None] == jnp.arange(devices, dtype=jnp.int32)[None, :]).astype(jnp.int32)
        return lax.optimization_barrier(jnp.sum((jnp.cumsum(onehot, axis=0) - onehot) * onehot, axis=1))
    ranking = lax.map(ranks_of, target.reshape(devices, BLK_DEV)).reshape(blocks)
    sender = jnp.arange(blocks, dtype=jnp.int32) // BLK_DEV
    brick_x = target // (N_GY * N_GZ)
    brick_y = target // N_GZ % N_GY
    brick_z = target % N_GZ
    plane_cells = (CY + 1) * (CZ + 1)
    local_x = cell_index // plane_cells
    local_y = cell_index // (CZ + 1) % (CY + 1)
    local_z = cell_index % (CZ + 1)
    global_x = (brick_x[:, None] * CX + local_x) % NCX
    global_y = (brick_y[:, None] * CY + local_y) % NCY
    global_z = (brick_z[:, None] * CZ + local_z) % NCZ
    flat_cell = ((global_x * NCY + global_y) * NCZ + global_z).reshape(-1)
    moving = jnp.transpose(velocity, (1, 0, 2)).reshape(3, -1)
    cell_count = NCX * NCY * NCZ
    counts = jax.ops.segment_sum(jnp.ones(flat_cell.shape, jnp.float32), flat_cell, num_segments=cell_count)
    moments = jnp.stack([jax.ops.segment_sum(moving[component], flat_cell, num_segments=cell_count) for component in range(3)])
    cell_means = moments / jnp.maximum(counts, 1.0)
    cell_flow = cell_means.reshape(3, NCX, NCY, NCZ)
    picked = rotation_axis[(global_x + grid_shift[0]) % APER, (global_y + grid_shift[1]) % APER, (global_z + grid_shift[2]) % APER].reshape(-1)
    direction = axis_table()[:, picked]
    local_flow = cell_means[:, flat_cell]
    relative = [moving[component] - local_flow[component] for component in range(3)]
    turned = rotate_about(direction, relative)
    updated = jnp.stack([local_flow[component] + turned[component] for component in range(3)])
    updated = jnp.transpose(updated.reshape(3, blocks, BROWS), (1, 0, 2))
    places = (target * devices + sender) * MOST + ranking
    placed = jnp.zeros((devices * devices * MOST, 3, BROWS), jnp.float32).at[places].set(updated)
    brick_velocity = placed.reshape(devices, devices, MOST, 3, BROWS)
    return (brick_velocity, cell_flow)
```

```python
import functools
import jax
import jax.numpy as jnp
import numpy as np
from jax import lax
from jax.experimental import pallas as pl
from jax.experimental.pallas import tpu as pltpu
from jax.sharding import PartitionSpec as P

CX = 4
CY = 8
CZ = 128
NAX = 64
APER = 32
EY = CY + 1
PLANES = (CX + 1) * EY
AXES = ("gx", "gy", "gz")
MESH_ID = pl.DeviceIdType.MESH

RIM = CY - 1
LOW = RIM + 1
HIGH = RIM + 2
SIDE = RIM + 3
INNER = SIDE + CX - 1
TILES = INNER + ((CX - 1) * (CY - 1) + 1) // 2
WIDE = 2 * CZ
STEP = 8

angle_cosine = -0.6427876096865393
angle_sine = 0.766044443118978


def axis_rows():
    counter = np.arange(NAX) + 0.5
    height = 1.0 - 2.0 * counter / NAX
    radius = np.sqrt(np.maximum(1.0 - height * height, 0.0))
    turning = counter * 2.399963229728653
    rows = np.zeros((8, 128), np.float32)
    rows[0, :NAX] = radius * np.cos(turning)
    rows[1, :NAX] = radius * np.sin(turning)
    rows[2, :NAX] = height
    return rows


def rotate_about(direction, relative):
    inner_product = (
        direction[0] * relative[0] + direction[1] * relative[1] + direction[2] * relative[2]
    )
    crossed = [
        direction[1] * relative[2] - direction[2] * relative[1],
        direction[2] * relative[0] - direction[0] * relative[2],
        direction[0] * relative[1] - direction[1] * relative[0],
    ]
    return [
        relative[component] * angle_cosine
        + crossed[component] * angle_sine
        + direction[component] * inner_product * (1.0 - angle_cosine)
        for component in range(3)
    ]


def take_lanes(values, index):
    return jnp.take_along_axis(values, index, axis=1, mode="promise_in_bounds")


def row_of_plane(ex, ey):
    static = isinstance(ex, int)
    where = (lambda c, a, b: a if c else b) if static else jnp.where
    inner = 2 * INNER + (ex - 1) * (CY - 1) + ey - 1
    last_x = ex == CX
    last_y = ey == CY
    half_x = where(last_x, 1, 0)
    half_y = where(last_y, 1, 0)
    corner = 2 * (LOW + half_y) + half_x
    side_x = 2 * (ey - 1) + half_x
    side_y = 2 * (SIDE + ex - 1) + half_y
    edge_x = (ex == 0) | last_x
    edge_y = (ey == 0) | last_y
    return where(
        edge_x, where(edge_y, corner, side_x), where(edge_y, side_y, inner)
    )


def position_codes(cell):
    plane = (cell * 8129) >> 20
    depth = cell - plane * (CZ + 1)
    ex = (plane * 57) >> 9
    ey = plane - ex * EY
    main = row_of_plane(ex, ey) * 128 + depth
    rim = 2 * RIM * 128 + plane
    return jnp.where(depth == CZ, rim, jnp.where(depth == 0, rim + 128, main))


def neighbours(sizes):
    steps = [(0, 1) if size == 2 else (0, 1, -1) for size in sizes]
    return [
        (dx, dy, dz)
        for dx in steps[0]
        for dy in steps[1]
        for dz in steps[2]
        if (dx, dy, dz) != (0, 0, 0)
    ]


def halo_tiles(step):
    if step[2] != 0:
        return RIM, LOW
    if step[0] != 0:
        return (RIM, SIDE) if step[1] != 0 else (0, SIDE)
    return RIM, INNER


def exchange_kernel(
    sizes,
    room,
    shift_ref,
    target_ref,
    velocity_ref,
    cell_ref,
    rotation_ref,
    recv_ref,
    table_ref,
    send_ref,
    total_ref,
    tile_ref,
    halo_ref,
    block_ref,
    plane_ref,
    kind_ref,
    send_sem,
    recv_sem,
    halo_send_sem,
    halo_recv_sem,
):
    nx, ny, nz = sizes
    devices = nx * ny * nz
    blocks = velocity_ref.shape[1]
    per = 4 * room
    place = tuple(lax.axis_index(axis) for axis in AXES)
    me = (place[0] * ny + place[1]) * nz + place[2]

    def away(k, sign):
        ox, oy, oz = k // (ny * nz), k // nz % ny, k % nz
        there = (
            (place[0] + sign * ox + nx) % nx,
            (place[1] + sign * oy + ny) % ny,
            (place[2] + sign * oz + nz) % nz,
        )
        return there, (there[0] * ny + there[1]) * nz + there[2]

    barrier = pltpu.get_barrier_semaphore()

    def greet(k, carry):
        there, number = away(k, 1)
        pl.semaphore_signal(barrier, inc=1, device_id=there, device_id_type=MESH_ID)
        return carry

    lax.fori_loop(1, devices, greet, 0)

    target = target_ref[...]
    named = (lax.broadcasted_iota(jnp.int32, (devices, blocks), 0) == target).astype(jnp.float32)
    earlier = (
        lax.broadcasted_iota(jnp.int32, (blocks, blocks), 0)
        < lax.broadcasted_iota(jnp.int32, (blocks, blocks), 1)
    ).astype(jnp.float32)
    before = jnp.dot(
        named.astype(jnp.bfloat16), earlier.astype(jnp.bfloat16), preferred_element_type=jnp.float32
    )
    rank = jnp.sum(named * before, axis=0, keepdims=True).astype(jnp.int32)
    slot = target * room + rank
    chosen = (
        (lax.broadcasted_iota(jnp.int32, (devices * room, blocks), 0) == slot)
        .astype(jnp.float32)
        .astype(jnp.bfloat16)
    )
    codes = position_codes(cell_ref[...]).astype(jnp.float32)
    for channel in range(4):
        left = codes if channel == 0 else velocity_ref[channel - 1]
        placed = None
        for part in range(3):
            upper = left.astype(jnp.bfloat16)
            moved = jnp.dot(chosen, upper, preferred_element_type=jnp.float32)
            placed = moved if placed is None else placed + moved
            left = left - upper.astype(jnp.float32)
        send_ref[pl.ds(channel, devices * room, stride=4), :] = placed

    lane = lax.broadcasted_iota(jnp.int32, (APER, 128), 1)
    depth_index = (lane + place[2] * CZ + shift_ref[2]) % APER
    for ex in range(CX + 1):
        index_x = ((place[0] * CX + ex) % (CX * nx) + shift_ref[0]) % APER
        layer = rotation_ref[index_x].astype(jnp.float32)
        layer = jnp.concatenate([layer] * (128 // APER), axis=1)
        block_ref[ex * APER : (ex + 1) * APER, :] = take_lanes(layer, depth_index)
        for ey in range(EY):
            index_y = ((place[1] * CY + ey) % (CY * ny) + shift_ref[1]) % APER
            row = block_ref[pl.ds(ex * APER + index_y, 1), :]
            plane_ref[ex * EY + ey : ex * EY + ey + 1, :] = row
            at = row_of_plane(ex, ey)
            kind_ref[at // 2, at % 2 : at % 2 + 1, :] = row
    planes = plane_ref[0 : 8 * (PLANES // 8 + 1), :]
    sublane = lax.broadcasted_iota(jnp.int32, planes.shape, 0)
    lanes = lax.broadcasted_iota(jnp.int32, planes.shape, 1)
    first = take_lanes(planes, jnp.zeros(planes.shape, jnp.int32))
    rim_kind = jnp.sum(
        jnp.where((sublane == lanes) & (sublane < PLANES), first, 0.0), axis=0, keepdims=True
    )
    kind_ref[RIM, 0:1, :] = rim_kind
    kind_ref[RIM, 1:2, :] = rim_kind
    kind_ref[TILES - 1, 1:2, :] = jnp.zeros((1, 128), jnp.float32)

    pl.semaphore_wait(barrier, devices - 1)

    def outgoing(k):
        there, number = away(k, 1)
        return pltpu.make_async_remote_copy(
            src_ref=send_ref.at[pl.ds(pl.multiple_of(number * per, 8), per), :],
            dst_ref=recv_ref.at[pl.ds(pl.multiple_of(me * per, 8), per), :],
            send_sem=send_sem.at[k],
            recv_sem=recv_sem.at[k],
            device_id=there,
            device_id_type=MESH_ID,
        )

    def start(k, carry):
        outgoing(k).start()
        return carry

    lax.fori_loop(1, devices, start, 0)
    own = pl.ds(pl.multiple_of(me * per, 8), per)
    recv_ref[own, :] = send_ref[own, :]
    total_ref[...] = jnp.zeros(total_ref.shape, jnp.float32)
    half = lax.broadcasted_iota(jnp.int32, (8, 128), 0)

    def add_sender(k, carry):
        _, number = away(k, -1)
        base = pl.multiple_of(number * per, 8)

        @pl.when(k > 0)
        def arrived():
            pltpu.make_async_remote_copy(
                src_ref=recv_ref.at[pl.ds(base, per), :],
                dst_ref=recv_ref.at[pl.ds(base, per), :],
                send_sem=send_sem.at[k],
                recv_sem=recv_sem.at[k],
                device_id=place,
                device_id_type=MESH_ID,
            ).wait_recv()

        by_row = lax.broadcasted_iota(jnp.int32, (8 * TILES, 128), 0) >> 3
        by_column = lax.broadcasted_iota(jnp.int32, (WIDE, 128), 0)
        lefts, rights = [], []
        for pair in range(room // 2):
            data = recv_ref[pl.ds(base + 8 * pair, 8), :]
            upper = data.astype(jnp.bfloat16).astype(jnp.float32)
            lower = data - upper
            whole = data.astype(jnp.int32)
            for which in range(2):
                if which == 0:
                    values = jnp.where(half < 4, upper, pltpu.roll(lower, 4, 0))
                else:
                    values = jnp.where(half < 4, pltpu.roll(upper, 4, 0), lower)
                values = jnp.where(half == 0, 1.0, jnp.where(half == 4, 0.0, values))
                code = whole[4 * which : 4 * which + 1]
                tiled = jnp.concatenate([values] * TILES, axis=0)
                lefts.append(jnp.where(by_row == code >> 8, tiled, 0.0).astype(jnp.bfloat16))
                rights.append(
                    (by_column == (code & (WIDE - 1))).astype(jnp.float32).astype(jnp.bfloat16)
                )
        middle = room // 2
        for part, span in enumerate((slice(0, middle), slice(middle, room))):
            total_ref[part] += lax.dot_general(
                jnp.concatenate(lefts[span], axis=1),
                jnp.concatenate(rights[span], axis=1),
                (((1,), (1,)), ((), ())),
                preferred_element_type=jnp.float32,
            )
        return carry

    lax.fori_loop(0, devices, add_sender, 0)

    for tile in range(TILES):
        rows = pl.ds(8 * tile, 8)
        value = total_ref[0, rows, :] + total_ref[1, rows, :]
        value = value + pltpu.roll(value, 4, 0)
        tile_ref[tile] = jnp.where(half < 4, value[:, :CZ], value[:, CZ:])

    steps = neighbours(sizes)

    def slot_of(step):
        return steps.index(
            tuple(abs(d) if size == 2 else d for d, size in zip(step, sizes))
        )

    copies = []
    for step in steps:
        low, high = halo_tiles(step)
        there = tuple((p + d + size) % size for p, d, size in zip(place, step, sizes))
        landing = slot_of(tuple(-d for d in step))
        copies.append(
            pltpu.make_async_remote_copy(
                src_ref=tile_ref.at[low:high],
                dst_ref=halo_ref.at[landing, 0 : high - low],
                send_sem=halo_send_sem.at[slot_of(step)],
                recv_sem=halo_recv_sem.at[landing],
                device_id=there,
                device_id_type=MESH_ID,
            )
        )
    for copy in copies:
        copy.start()

    def sent(k, carry):
        outgoing(k).wait_send()
        return carry

    lax.fori_loop(1, devices, sent, 0)
    for copy in copies:
        copy.wait()

    def got(step, tile):
        low, high = halo_tiles(step)
        return halo_ref[slot_of(step), tile - low]

    def turned(step, tile):
        return pltpu.roll(got(step, tile), 4, 0)

    def both(low, high):
        return jnp.where(half < 4, low, high)

    lane = lax.broadcasted_iota(jnp.int32, (8, 128), 1)
    plane_x = (lane * 57) >> 9
    plane_y = lane - plane_x * EY

    def rim(dx, dy):
        own_rim = tile_ref[RIM] if (dx, dy) == (0, 0) else got((dx, dy, 0), RIM)
        return own_rim + both(turned((dx, dy, 1), RIM), turned((dx, dy, -1), RIM))

    for tile in range(TILES):
        value = tile_ref[tile]
        if tile < RIM or tile in (LOW, HIGH):
            value = value + both(turned((-1, 0, 0), tile), turned((1, 0, 0), tile))
        if tile in (LOW, HIGH):
            dy, other = (-1, HIGH) if tile == LOW else (1, LOW)
            value = value + got((0, dy, 0), other)
            value = value + both(turned((-1, dy, 0), other), turned((1, dy, 0), other))
        if SIDE <= tile < INNER:
            value = value + both(turned((0, -1, 0), tile), turned((0, 1, 0), tile))
        if tile == RIM:
            value = rim(0, 0)
            for dx in (-1, 0, 1):
                for dy in (-1, 0, 1):
                    if (dx, dy) == (0, 0):
                        continue
                    inside = lane < PLANES
                    if dx != 0:
                        inside = inside & (plane_x == (CX if dx > 0 else 0))
                    if dy != 0:
                        inside = inside & (plane_y == (CY if dy > 0 else 0))
                    moved = pltpu.roll(rim(dx, dy), (dx * CX * EY + dy * CY) % 128, 1)
                    value = value + jnp.where(inside, moved, 0.0)
        count = both(
            jnp.broadcast_to(value[0:1], (8, 128)), jnp.broadcast_to(value[4:5], (8, 128))
        )
        mean = value / jnp.maximum(count, 1.0)
        kind = both(
            jnp.broadcast_to(kind_ref[tile, 0:1, :], (8, 128)),
            jnp.broadcast_to(kind_ref[tile, 1:2, :], (8, 128)),
        )
        table_ref[8 * tile : 8 * tile + 8, :] = jnp.where(half % 4 == 0, kind, mean)


def update_kernel(slots, room, recv_ref, table_ref, axis_ref, out_ref, flow_ref, held_ref):
    devices = out_ref.shape[2]
    per = 4 * room
    groups = devices // STEP
    for channel in range(4):
        value = jnp.concatenate(
            [
                table_ref[pl.ds(channel, TILES, stride=8), :],
                table_ref[pl.ds(channel + 4, TILES, stride=8), :],
            ],
            axis=1,
        )
        upper = value.astype(jnp.bfloat16)
        held_ref[channel * TILES : (channel + 1) * TILES, :] = upper
        if channel > 0:
            held_ref[(channel + 3) * TILES : (channel + 4) * TILES, :] = (
                value - upper.astype(jnp.float32)
            ).astype(jnp.bfloat16)

    sublane = lax.broadcasted_iota(jnp.int32, (CY, 128), 0)
    lane = lax.broadcasted_iota(jnp.int32, (CY, 128), 1)
    for component in range(3):
        rim = table_ref[8 * RIM + 5 + component : 8 * RIM + 6 + component, :]
        rim = jnp.broadcast_to(rim, (CY, 128))
        for ex in range(CX):
            rows = []
            for ey in range(CY):
                at = 4 * row_of_plane(ex, ey) + 1 + component
                rows.append(table_ref[at : at + 1, :])
            flow = jnp.concatenate(rows, axis=0)
            edge = take_lanes(rim, sublane + ex * EY)
            flow_ref[component, ex] = jnp.where(lane == 0, edge, flow)

    by_row = lax.broadcasted_iota(jnp.int32, (TILES, 2 * 128), 0)
    by_column = lax.broadcasted_iota(jnp.int32, (WIDE, 2 * 128), 0)

    def step(i, carry):
        rank = i // groups
        sender = (i % groups) * STEP
        blocks = [
            recv_ref[pl.ds((sender + j) * per + 4 * rank, 4), :] for j in range(STEP)
        ]
        picked = [[] for channel in range(4)]
        for j in range(0, STEP, 2):
            code = jnp.concatenate([blocks[j][0:1], blocks[j + 1][0:1]], axis=1).astype(jnp.int32)
            onehot = (by_column == (code & (WIDE - 1))).astype(jnp.float32).astype(jnp.bfloat16)
            read = jnp.dot(held_ref[...], onehot, preferred_element_type=jnp.float32)
            here = by_row == code >> 8
            for channel in range(4):
                value = read[channel * TILES : (channel + 1) * TILES]
                if channel > 0:
                    value = value + read[(channel + 3) * TILES : (channel + 4) * TILES]
                row = jnp.sum(jnp.where(here, value, 0.0), axis=0, keepdims=True)
                picked[channel] += [row[:, :128], row[:, 128:]]
        held = [jnp.concatenate(rows, axis=0) for rows in picked]
        own = [jnp.concatenate([block[c : c + 1] for block in blocks], axis=0) for c in range(4)]
        kind = held[0].astype(jnp.int32)
        direction = [
            take_lanes(jnp.broadcast_to(axis_ref[c : c + 1, :], (STEP, 128)), kind)
            for c in range(3)
        ]
        relative = [own[c + 1] - held[c + 1] for c in range(3)]
        turned = rotate_about(direction, relative)
        there = pl.ds(pl.multiple_of(sender, STEP), STEP)
        for c in range(3):
            out_ref[rank, c, there, :] = held[c + 1] + turned[c]
        return carry

    lax.fori_loop(0, slots * groups, step, 0)


def shards(velocity, cell_index, block_target, rotation_axis, grid_shift):
    sizes = tuple(lax.axis_size(axis) for axis in AXES)
    devices = sizes[0] * sizes[1] * sizes[2]
    blocks = velocity.shape[0]
    lanes = velocity.shape[2]
    slots = 3 * blocks // (2 * devices)
    room = slots + slots % 2
    count = len(neighbours(sizes))
    vmem = pl.BlockSpec(memory_space=pltpu.VMEM)
    arrived, table = pl.pallas_call(
        functools.partial(exchange_kernel, sizes, room),
        out_shape=[
            jax.ShapeDtypeStruct((devices * room * 4, lanes), jnp.float32),
            jax.ShapeDtypeStruct((8 * TILES, lanes), jnp.float32),
        ],
        in_specs=[pl.BlockSpec(memory_space=pltpu.SMEM), vmem, vmem, vmem, vmem],
        out_specs=[vmem, vmem],
        scratch_shapes=[
            pltpu.VMEM((devices * room * 4, lanes), jnp.float32),
            pltpu.VMEM((2, 8 * TILES, WIDE), jnp.float32),
            pltpu.VMEM((TILES, 8, lanes), jnp.float32),
            pltpu.VMEM((count, SIDE, 8, lanes), jnp.float32),
            pltpu.VMEM(((CX + 1) * APER, lanes), jnp.float32),
            pltpu.VMEM((8 * (PLANES // 8 + 1), lanes), jnp.float32),
            pltpu.VMEM((TILES, 8, lanes), jnp.float32),
            pltpu.SemaphoreType.DMA((devices,)),
            pltpu.SemaphoreType.DMA((devices,)),
            pltpu.SemaphoreType.DMA((count,)),
            pltpu.SemaphoreType.DMA((count,)),
        ],
        compiler_params=pltpu.CompilerParams(collective_id=0, has_side_effects=True),
        cost_estimate=pl.CostEstimate(flops=1 << 33, bytes_accessed=1 << 21, transcendentals=0),
    )(
        grid_shift,
        block_target.reshape(1, blocks),
        jnp.transpose(velocity, (1, 0, 2)),
        cell_index,
        rotation_axis,
    )
    updated, flow = pl.pallas_call(
        functools.partial(update_kernel, slots, room),
        out_shape=[
            jax.ShapeDtypeStruct((slots, 3, devices, lanes), jnp.float32),
            jax.ShapeDtypeStruct((3, CX, CY, CZ), jnp.float32),
        ],
        in_specs=[vmem, vmem, vmem],
        out_specs=[vmem, vmem],
        scratch_shapes=[pltpu.VMEM((7 * TILES, WIDE), jnp.bfloat16)],
        cost_estimate=pl.CostEstimate(flops=1 << 33, bytes_accessed=1 << 21, transcendentals=0),
    )(arrived, table, jnp.asarray(axis_rows()))
    return (jnp.transpose(updated, (2, 0, 1, 3))[None], flow)


def solution(mesh):
    return jax.shard_map(
        shards,
        mesh=mesh,
        in_specs=(
            P(AXES, None, None),
            P(AXES, None),
            P(AXES, None),
            P(),
            P(),
        ),
        out_specs=(P(AXES, None, None, None, None), P(None, "gx", "gy", "gz")),
        check_vma=False,
    )
```

```python
import functools
import jax
import jax.numpy as jnp
import numpy as np
from jax import lax
from jax.experimental import pallas as pl
from jax.experimental.pallas import tpu as pltpu
from jax.sharding import PartitionSpec as P

CX = 4
CY = 8
CZ = 128
NAX = 64
APER = 32
EY = CY + 1
PLANES = (CX + 1) * EY
AXES = ("gx", "gy", "gz")
MESH_ID = pl.DeviceIdType.MESH

RIM = CY - 1
LOW = RIM + 1
HIGH = RIM + 2
SIDE = RIM + 3
INNER = SIDE + CX - 1
TILES = INNER + ((CX - 1) * (CY - 1) + 1) // 2
WIDE = 2 * CZ
BOUND = 2 * INNER
ROWS = BOUND + (CX - 1) * (CY - 1)

angle_cosine = -0.6427876096865393
angle_sine = 0.766044443118978


def axis_rows():
    counter = np.arange(NAX) + 0.5
    height = 1.0 - 2.0 * counter / NAX
    radius = np.sqrt(np.maximum(1.0 - height * height, 0.0))
    turning = counter * 2.399963229728653
    rows = np.zeros((8, 128), np.float32)
    rows[0, :NAX] = radius * np.cos(turning)
    rows[1, :NAX] = radius * np.sin(turning)
    rows[2, :NAX] = height
    return rows


def rotate_about(direction, relative):
    inner_product = (
        direction[0] * relative[0] + direction[1] * relative[1] + direction[2] * relative[2]
    )
    crossed = [
        direction[1] * relative[2] - direction[2] * relative[1],
        direction[2] * relative[0] - direction[0] * relative[2],
        direction[0] * relative[1] - direction[1] * relative[0],
    ]
    return [
        relative[component] * angle_cosine
        + crossed[component] * angle_sine
        + direction[component] * inner_product * (1.0 - angle_cosine)
        for component in range(3)
    ]


def take_lanes(values, index):
    return jnp.take_along_axis(values, index, axis=1, mode="promise_in_bounds")


def row_of_plane(ex, ey):
    static = isinstance(ex, int)
    where = (lambda c, a, b: a if c else b) if static else jnp.where
    inner = 2 * INNER + (ex - 1) * (CY - 1) + ey - 1
    last_x = ex == CX
    last_y = ey == CY
    half_x = where(last_x, 1, 0)
    half_y = where(last_y, 1, 0)
    corner = 2 * (LOW + half_y) + half_x
    side_x = 2 * (ey - 1) + half_x
    side_y = 2 * (SIDE + ex - 1) + half_y
    edge_x = (ex == 0) | last_x
    edge_y = (ey == 0) | last_y
    return where(
        edge_x, where(edge_y, corner, side_x), where(edge_y, side_y, inner)
    )


def position_codes(cell):
    plane = (cell * 8129) >> 20
    depth = cell - plane * (CZ + 1)
    ex = (plane * 57) >> 9
    ey = plane - ex * EY
    main = row_of_plane(ex, ey) * 128 + depth
    rim = 2 * RIM * 128 + plane
    return jnp.where(depth == CZ, rim, jnp.where(depth == 0, rim + 128, main))


def neighbours(sizes):
    steps = [(0, 1) if size == 2 else (0, 1, -1) for size in sizes]
    return [
        (dx, dy, dz)
        for dx in steps[0]
        for dy in steps[1]
        for dz in steps[2]
        if (dx, dy, dz) != (0, 0, 0)
    ]


def halo_tiles(step):
    if step[2] != 0:
        return RIM, LOW
    if step[0] != 0:
        return (RIM, SIDE) if step[1] != 0 else (0, SIDE)
    return RIM, INNER


def exchange_kernel(
    sizes,
    slots,
    room,
    shift_hbm,
    target_hbm,
    velocity_hbm,
    cell_hbm,
    rotation_hbm,
    axis_hbm,
    base_ref,
    code_ref,
    table_ref,
    pull_ref,
    shift_ref,
    target_ref,
    velocity_ref,
    cell_ref,
    rotation_ref,
    axis_ref,
    recv_ref,
    send_ref,
    total_ref,
    tile_ref,
    halo_ref,
    block_ref,
    plane_ref,
    kind_ref,
    direction_ref,
    load_sem,
    send_sem,
    recv_sem,
    halo_send_sem,
    halo_recv_sem,
):
    nx, ny, nz = sizes
    devices = nx * ny * nz
    half_y = ny // 2
    blocks = velocity_ref.shape[1]
    per = 4 * room
    place = tuple(lax.axis_index(axis) for axis in AXES)
    me = (place[0] * ny + place[1]) * nz + place[2]

    loads = [
        pltpu.make_async_copy(source, sink, load_sem.at[i])
        for i, (source, sink) in enumerate(
            (
                (target_hbm, target_ref),
                (cell_hbm, cell_ref),
                (velocity_hbm, velocity_ref),
                (shift_hbm, shift_ref),
                (rotation_hbm, rotation_ref),
                (axis_hbm, axis_ref),
            )
        )
    ]
    for load in loads:
        load.start()

    def wrap(value, size):
        return jnp.where(value >= size, value - size, value)

    low_y = place[1] % half_y
    base_y = place[1] - low_y

    def partner(k, sign):
        q = k // 2
        ox, oy, oz = q // (nz * half_y), q // nz % half_y, q % nz
        if sign < 0:
            ox, oy, oz = nx - ox, half_y - oy, nz - oz
        other = half_y * (k % 2)
        there = (
            wrap(place[0] + ox, nx),
            wrap(base_y + other, ny) + wrap(low_y + oy, half_y),
            wrap(place[2] + oz, nz),
        )
        return there, (there[0] * ny + there[1]) * nz + there[2]

    barrier = pltpu.get_barrier_semaphore()
    for k in range(1, devices):
        pl.semaphore_signal(
            barrier, inc=1, device_id=partner(k, 1)[0], device_id_type=MESH_ID
        )

    loads[0].wait()
    target = target_ref[...]
    named = (lax.broadcasted_iota(jnp.int32, (devices, blocks), 0) == target).astype(jnp.float32)
    earlier = (
        lax.broadcasted_iota(jnp.int32, (blocks, blocks), 0)
        < lax.broadcasted_iota(jnp.int32, (blocks, blocks), 1)
    ).astype(jnp.float32)
    before = jnp.dot(
        named.astype(jnp.bfloat16), earlier.astype(jnp.bfloat16), preferred_element_type=jnp.float32
    )
    rank = jnp.sum(named * before, axis=0, keepdims=True).astype(jnp.int32)
    slot = target * room + rank
    chosen = (
        (lax.broadcasted_iota(jnp.int32, (devices * room, blocks), 0) == slot)
        .astype(jnp.float32)
        .astype(jnp.bfloat16)
    )
    loads[1].wait()
    codes = position_codes(cell_ref[...]).astype(jnp.float32)
    loads[2].wait()
    for channel in range(4):
        left = codes if channel == 0 else velocity_ref[channel - 1]
        placed = None
        for part in range(3):
            upper = left.astype(jnp.bfloat16)
            moved = jnp.dot(chosen, upper, preferred_element_type=jnp.float32)
            placed = moved if placed is None else placed + moved
            left = left - upper.astype(jnp.float32)
        send_ref[pl.ds(channel, devices * room, stride=4), :] = placed

    for load in loads[3:]:
        load.wait()
    lane = lax.broadcasted_iota(jnp.int32, (APER, 128), 1)
    depth_index = (lane + place[2] * CZ + shift_ref[2]) % APER
    for ex in range(CX + 1):
        index_x = ((place[0] * CX + ex) % (CX * nx) + shift_ref[0]) % APER
        layer = rotation_ref[index_x].astype(jnp.float32)
        layer = jnp.concatenate([layer] * (128 // APER), axis=1)
        block_ref[ex * APER : (ex + 1) * APER, :] = take_lanes(layer, depth_index)
        for ey in range(EY):
            index_y = ((place[1] * CY + ey) % (CY * ny) + shift_ref[1]) % APER
            row = block_ref[pl.ds(ex * APER + index_y, 1), :]
            plane_ref[ex * EY + ey : ex * EY + ey + 1, :] = row
            at = row_of_plane(ex, ey)
            kind_ref[at : at + 1, :] = row
    planes = plane_ref[0 : 8 * (PLANES // 8 + 1), :]
    sublane = lax.broadcasted_iota(jnp.int32, planes.shape, 0)
    lanes = lax.broadcasted_iota(jnp.int32, planes.shape, 1)
    first = take_lanes(planes, jnp.zeros(planes.shape, jnp.int32))
    rim_kind = jnp.sum(
        jnp.where((sublane == lanes) & (sublane < PLANES), first, 0.0), axis=0, keepdims=True
    )
    kind_ref[2 * RIM : 2 * RIM + 1, :] = rim_kind
    kind_ref[2 * RIM + 1 : 2 * RIM + 2, :] = rim_kind
    kind_ref[ROWS : 2 * TILES, :] = jnp.zeros((2 * TILES - ROWS, 128), jnp.float32)
    kinds = kind_ref[...].astype(jnp.int32)
    for component in range(3):
        direction_ref[component] = take_lanes(
            jnp.broadcast_to(axis_ref[component : component + 1, :], kinds.shape), kinds
        )

    pl.semaphore_wait(barrier, devices - 1)

    def outgoing(k):
        there, number = partner(k, 1)
        return pltpu.make_async_remote_copy(
            src_ref=send_ref.at[pl.ds(pl.multiple_of(number * per, 8), per), :],
            dst_ref=recv_ref.at[pl.ds(pl.multiple_of(me * per, 8), per), :],
            send_sem=send_sem.at[k],
            recv_sem=recv_sem.at[k],
            device_id=there,
            device_id_type=MESH_ID,
        )

    for k in range(1, devices):
        outgoing(k).start()
    own = pl.ds(pl.multiple_of(me * per, 8), per)
    recv_ref[own, :] = send_ref[own, :]
    total_ref[...] = jnp.zeros(total_ref.shape, jnp.float32)
    half = lax.broadcasted_iota(jnp.int32, (8, 128), 0)

    def select_rows(source, rows, row, lane, channels, start):
        found = [jnp.zeros(row.shape, jnp.float32) for c in range(channels)]
        for r in rows:
            here = row == r
            for c in range(channels):
                at = start(r, c)
                line = jnp.broadcast_to(source[at : at + 1, :], row.shape)
                found[c] = jnp.where(here, take_lanes(line, lane), found[c])
        return found

    firsts = [0] if room <= 8 else [*range(0, room - 7, 8)] + ([room - 8] if room % 8 else [])

    def add_sender(k, carry):
        _, number = partner(k, -1)
        base = pl.multiple_of(number * per, 8)

        @pl.when(k > 0)
        def arrived():
            pltpu.make_async_remote_copy(
                src_ref=recv_ref.at[pl.ds(base, per), :],
                dst_ref=recv_ref.at[pl.ds(base, per), :],
                send_sem=send_sem.at[k],
                recv_sem=recv_sem.at[k],
                device_id=place,
                device_id_type=MESH_ID,
            ).wait_recv()

        by_row = lax.broadcasted_iota(jnp.int32, (8 * TILES, 128), 0) >> 3
        by_column = lax.broadcasted_iota(jnp.int32, (WIDE, 128), 0)
        lefts, rights = [], []
        for pair in range(room // 2):
            data = recv_ref[pl.ds(base + 8 * pair, 8), :]
            upper = data.astype(jnp.bfloat16).astype(jnp.float32)
            lower = data - upper
            whole = data.astype(jnp.int32)
            for which in range(2):
                if which == 0:
                    values = jnp.where(half < 4, upper, pltpu.roll(lower, 4, 0))
                else:
                    values = jnp.where(half < 4, pltpu.roll(upper, 4, 0), lower)
                values = jnp.where(half == 0, 1.0, jnp.where(half == 4, 0.0, values))
                code = whole[4 * which : 4 * which + 1]
                tiled = jnp.concatenate([values] * TILES, axis=0)
                lefts.append(jnp.where(by_row == code >> 8, tiled, 0.0).astype(jnp.bfloat16))
                rights.append(
                    (by_column == (code & (WIDE - 1))).astype(jnp.float32).astype(jnp.bfloat16)
                )
        middle = room // 2
        for part, span in enumerate((slice(0, middle), slice(middle, room))):
            total_ref[part] += lax.dot_general(
                jnp.concatenate(lefts[span], axis=1),
                jnp.concatenate(rights[span], axis=1),
                (((1,), (1,)), ((), ())),
                preferred_element_type=jnp.float32,
            )

        for first in firsts:
            take = min(8, room)

            def rows_of(channel):
                rows = recv_ref[pl.ds(base + 4 * first + channel, take, stride=4), :]
                return jnp.concatenate([rows] * (8 // take), axis=0)

            code = rows_of(0).astype(jnp.int32)
            kind = select_rows(kind_ref, range(ROWS), code >> 7, code & 127, 1, lambda r, c: r)[0]
            kind = kind.astype(jnp.int32)
            direction = [
                take_lanes(jnp.broadcast_to(axis_ref[c : c + 1, :], (8, 128)), kind)
                for c in range(3)
            ]
            turned = rotate_about(direction, [rows_of(c + 1) for c in range(3)])
            code_ref[pl.ds(first * devices + number, take, stride=devices), :] = code[:take]
            for c in range(3):
                at = (3 * first + c) * devices + number
                base_ref[pl.ds(at, take, stride=3 * devices), :] = turned[c][:take]
        return carry

    lax.fori_loop(0, devices, add_sender, 0)

    for tile in range(TILES):
        rows = pl.ds(8 * tile, 8)
        value = total_ref[0, rows, :] + total_ref[1, rows, :]
        value = value + pltpu.roll(value, 4, 0)
        tile_ref[tile] = jnp.where(half < 4, value[:, :CZ], value[:, CZ:])

    steps = neighbours(sizes)

    def slot_of(step):
        return steps.index(
            tuple(abs(d) if size == 2 else d for d, size in zip(step, sizes))
        )

    copies = []
    for step in steps:
        low, high = halo_tiles(step)
        there = tuple(
            wrap(p + d % size, size) if d else p for p, d, size in zip(place, step, sizes)
        )
        landing = slot_of(tuple(-d for d in step))
        copies.append(
            pltpu.make_async_remote_copy(
                src_ref=tile_ref.at[low:high],
                dst_ref=halo_ref.at[landing, 0 : high - low],
                send_sem=halo_send_sem.at[slot_of(step)],
                recv_sem=halo_recv_sem.at[landing],
                device_id=there,
                device_id_type=MESH_ID,
            )
        )
    for copy in copies:
        copy.start()

    def both(low, high):
        return jnp.where(half < 4, low, high)

    def finish(tile, value):
        count = both(
            jnp.broadcast_to(value[0:1], (8, 128)), jnp.broadcast_to(value[4:5], (8, 128))
        )
        table_ref[8 * tile : 8 * tile + 8, :] = value / jnp.maximum(count, 1.0)

    def pulls(low, high):
        mean = [table_ref[pl.ds(4 * low + 1 + c, high - low, stride=4), :] for c in range(3)]
        direction = [direction_ref[c, low:high, :] for c in range(3)]
        turned = rotate_about(direction, mean)
        for c in range(3):
            pull_ref[pl.ds(4 * low + 1 + c, high - low, stride=4), :] = mean[c] - turned[c]

    for tile in range(INNER, TILES):
        finish(tile, tile_ref[tile])
    pulls(BOUND, 2 * TILES)
    groups = devices // 8

    def inner(s, carry):
        for g in range(groups):
            at = pl.multiple_of(s * devices, 8) + 8 * g
            code = code_ref[pl.ds(at, 8), :]
            found = select_rows(
                pull_ref, range(BOUND, ROWS), code >> 7, code & 127, 3, lambda r, c: 4 * r + 1 + c
            )
            for c in range(3):
                place_at = pl.ds(pl.multiple_of((3 * s + c) * devices, 8) + 8 * g, 8)
                base_ref[place_at, :] = base_ref[place_at, :] + found[c]
        return carry

    lax.fori_loop(0, slots, inner, 0)

    for k in range(1, devices):
        outgoing(k).wait_send()
    for copy in copies:
        copy.wait()

    def got(step, tile):
        low, high = halo_tiles(step)
        return halo_ref[slot_of(step), tile - low]

    def turned(step, tile):
        return pltpu.roll(got(step, tile), 4, 0)

    lane = lax.broadcasted_iota(jnp.int32, (8, 128), 1)
    plane_x = (lane * 57) >> 9
    plane_y = lane - plane_x * EY

    def rim(dx, dy):
        own_rim = tile_ref[RIM] if (dx, dy) == (0, 0) else got((dx, dy, 0), RIM)
        return own_rim + both(turned((dx, dy, 1), RIM), turned((dx, dy, -1), RIM))

    for tile in range(INNER):
        value = tile_ref[tile]
        if tile < RIM or tile in (LOW, HIGH):
            value = value + both(turned((-1, 0, 0), tile), turned((1, 0, 0), tile))
        if tile in (LOW, HIGH):
            dy, other = (-1, HIGH) if tile == LOW else (1, LOW)
            value = value + got((0, dy, 0), other)
            value = value + both(turned((-1, dy, 0), other), turned((1, dy, 0), other))
        if SIDE <= tile < INNER:
            value = value + both(turned((0, -1, 0), tile), turned((0, 1, 0), tile))
        if tile == RIM:
            value = rim(0, 0)
            for dx in (-1, 0, 1):
                for dy in (-1, 0, 1):
                    if (dx, dy) == (0, 0):
                        continue
                    inside = lane < PLANES
                    if dx != 0:
                        inside = inside & (plane_x == (CX if dx > 0 else 0))
                    if dy != 0:
                        inside = inside & (plane_y == (CY if dy > 0 else 0))
                    moved = pltpu.roll(rim(dx, dy), (dx * CX * EY + dy * CY) % 128, 1)
                    value = value + jnp.where(inside, moved, 0.0)
        finish(tile, value)
    pulls(0, BOUND)


def update_kernel(slots, base_ref, code_ref, table_ref, pull_ref, out_ref, flow_ref):
    devices = out_ref.shape[2]
    sublane = lax.broadcasted_iota(jnp.int32, (CY, 128), 0)
    lane = lax.broadcasted_iota(jnp.int32, (CY, 128), 1)
    for component in range(3):
        rim = table_ref[8 * RIM + 5 + component : 8 * RIM + 6 + component, :]
        rim = jnp.broadcast_to(rim, (CY, 128))
        for ex in range(CX):
            rows = []
            for ey in range(CY):
                at = 4 * row_of_plane(ex, ey) + 1 + component
                rows.append(table_ref[at : at + 1, :])
            flow = jnp.concatenate(rows, axis=0)
            edge = take_lanes(rim, sublane + ex * EY)
            flow_ref[component, ex] = jnp.where(lane == 0, edge, flow)

    def outer(s, carry):
        for g in range(devices // 8):
            code = code_ref[pl.ds(pl.multiple_of(s * devices, 8) + 8 * g, 8), :]
            row, depth = code >> 7, code & 127
            found = [jnp.zeros((8, 128), jnp.float32) for c in range(3)]
            for r in range(BOUND):
                here = row == r
                for c in range(3):
                    at = 4 * r + 1 + c
                    line = jnp.broadcast_to(pull_ref[at : at + 1, :], (8, 128))
                    found[c] = jnp.where(here, take_lanes(line, depth), found[c])
            for c in range(3):
                at = pl.multiple_of((3 * s + c) * devices, 8) + 8 * g
                out_ref[s, c, 8 * g : 8 * g + 8, :] = base_ref[pl.ds(at, 8), :] + found[c]
        return carry

    lax.fori_loop(0, slots, outer, 0)


def shards(velocity, cell_index, block_target, rotation_axis, grid_shift):
    sizes = tuple(lax.axis_size(axis) for axis in AXES)
    devices = sizes[0] * sizes[1] * sizes[2]
    blocks = velocity.shape[0]
    lanes = velocity.shape[2]
    slots = 3 * blocks // (2 * devices)
    room = slots + slots % 2
    count = len(neighbours(sizes))
    vmem = pl.BlockSpec(memory_space=pltpu.VMEM)
    hbm = pl.BlockSpec(memory_space=pltpu.HBM)
    handed = pl.pallas_call(
        functools.partial(exchange_kernel, sizes, slots, room),
        out_shape=[
            pltpu.VMEM((room * 3 * devices, lanes), jnp.float32),
            pltpu.VMEM((room * devices, lanes), jnp.int32),
            pltpu.VMEM((8 * TILES, lanes), jnp.float32),
            pltpu.VMEM((8 * TILES, lanes), jnp.float32),
        ],
        in_specs=[hbm] * 6,
        out_specs=[vmem] * 4,
        scratch_shapes=[
            pltpu.SMEM((3,), jnp.int32),
            pltpu.VMEM((1, blocks), jnp.int32),
            pltpu.VMEM((3, blocks, lanes), jnp.float32),
            pltpu.VMEM((blocks, lanes), jnp.int32),
            pltpu.VMEM((APER, APER, APER), jnp.int32),
            pltpu.VMEM((8, 128), jnp.float32),
            pltpu.VMEM((devices * room * 4, lanes), jnp.float32),
            pltpu.VMEM((devices * room * 4, lanes), jnp.float32),
            pltpu.VMEM((2, 8 * TILES, WIDE), jnp.float32),
            pltpu.VMEM((TILES, 8, lanes), jnp.float32),
            pltpu.VMEM((count, SIDE, 8, lanes), jnp.float32),
            pltpu.VMEM(((CX + 1) * APER, lanes), jnp.float32),
            pltpu.VMEM((8 * (PLANES // 8 + 1), lanes), jnp.float32),
            pltpu.VMEM((2 * TILES, lanes), jnp.float32),
            pltpu.VMEM((3, 2 * TILES, lanes), jnp.float32),
            pltpu.SemaphoreType.DMA((6,)),
            pltpu.SemaphoreType.DMA((devices,)),
            pltpu.SemaphoreType.DMA((devices,)),
            pltpu.SemaphoreType.DMA((count,)),
            pltpu.SemaphoreType.DMA((count,)),
        ],
        compiler_params=pltpu.CompilerParams(collective_id=0, has_side_effects=True),
        cost_estimate=pl.CostEstimate(flops=1 << 33, bytes_accessed=1 << 21, transcendentals=0),
    )(
        grid_shift,
        block_target.reshape(1, blocks),
        jnp.transpose(velocity, (1, 0, 2)),
        cell_index,
        rotation_axis,
        jnp.asarray(axis_rows()),
    )
    updated, flow = pl.pallas_call(
        functools.partial(update_kernel, slots),
        out_shape=[
            jax.ShapeDtypeStruct((slots, 3, devices, lanes), jnp.float32),
            jax.ShapeDtypeStruct((3, CX, CY, CZ), jnp.float32),
        ],
        in_specs=[vmem] * 4,
        out_specs=[vmem, vmem],
        cost_estimate=pl.CostEstimate(flops=1 << 33, bytes_accessed=1 << 21, transcendentals=0),
    )(*[pltpu.with_memory_space_constraint(array, pltpu.VMEM) for array in handed])
    return (jnp.transpose(updated, (2, 0, 1, 3))[None], flow)


def solution(mesh):
    return jax.shard_map(
        shards,
        mesh=mesh,
        in_specs=(
            P(AXES, None, None),
            P(AXES, None),
            P(AXES, None),
            P(),
            P(),
        ),
        out_specs=(P(AXES, None, None, None, None), P(None, "gx", "gy", "gz")),
        check_vma=False,
    )
```

```python
import functools
import jax
import jax.numpy as jnp
import numpy as np
from jax import lax
from jax.experimental import pallas as pl
from jax.experimental.pallas import tpu as pltpu
from jax.sharding import PartitionSpec as P

CX = 4
CY = 8
CZ = 128
NAX = 64
APER = 32
EY = CY + 1
PLANES = (CX + 1) * EY
AXES = ("gx", "gy", "gz")
MESH_ID = pl.DeviceIdType.MESH

RIM = CY - 1
LOW = RIM + 1
HIGH = RIM + 2
SIDE = RIM + 3
INNER = SIDE + CX - 1
TILES = INNER + ((CX - 1) * (CY - 1) + 1) // 2
WIDE = 2 * CZ
BOUND = 2 * INNER
ROWS = BOUND + (CX - 1) * (CY - 1)

angle_cosine = -0.6427876096865393
angle_sine = 0.766044443118978


def axis_rows():
    counter = np.arange(NAX) + 0.5
    height = 1.0 - 2.0 * counter / NAX
    radius = np.sqrt(np.maximum(1.0 - height * height, 0.0))
    turning = counter * 2.399963229728653
    rows = np.zeros((8, 128), np.float32)
    rows[0, :NAX] = radius * np.cos(turning)
    rows[1, :NAX] = radius * np.sin(turning)
    rows[2, :NAX] = height
    return rows


def rotate_about(direction, relative):
    inner_product = (
        direction[0] * relative[0] + direction[1] * relative[1] + direction[2] * relative[2]
    )
    crossed = [
        direction[1] * relative[2] - direction[2] * relative[1],
        direction[2] * relative[0] - direction[0] * relative[2],
        direction[0] * relative[1] - direction[1] * relative[0],
    ]
    return [
        relative[component] * angle_cosine
        + crossed[component] * angle_sine
        + direction[component] * inner_product * (1.0 - angle_cosine)
        for component in range(3)
    ]


def take_lanes(values, index):
    return jnp.take_along_axis(values, index, axis=1, mode="promise_in_bounds")


def row_of_plane(ex, ey):
    static = isinstance(ex, int)
    where = (lambda c, a, b: a if c else b) if static else jnp.where
    inner = 2 * INNER + (ex - 1) * (CY - 1) + ey - 1
    last_x = ex == CX
    last_y = ey == CY
    half_x = where(last_x, 1, 0)
    half_y = where(last_y, 1, 0)
    corner = 2 * (LOW + half_y) + half_x
    side_x = 2 * (ey - 1) + half_x
    side_y = 2 * (SIDE + ex - 1) + half_y
    edge_x = (ex == 0) | last_x
    edge_y = (ey == 0) | last_y
    return where(
        edge_x, where(edge_y, corner, side_x), where(edge_y, side_y, inner)
    )


def position_codes(cell):
    plane = (cell * 8129) >> 20
    depth = cell - plane * (CZ + 1)
    ex = (plane * 57) >> 9
    ey = plane - ex * EY
    main = row_of_plane(ex, ey) * 128 + depth
    rim = 2 * RIM * 128 + plane
    return jnp.where(depth == CZ, rim, jnp.where(depth == 0, rim + 128, main))


def neighbours(sizes):
    steps = [(0, 1) if size == 2 else (0, 1, -1) for size in sizes]
    return [
        (dx, dy, dz)
        for dx in steps[0]
        for dy in steps[1]
        for dz in steps[2]
        if (dx, dy, dz) != (0, 0, 0)
    ]


def halo_tiles(step):
    if step[2] != 0:
        return RIM, LOW
    if step[0] != 0:
        return (RIM, SIDE) if step[1] != 0 else (0, SIDE)
    return RIM, INNER


def exchange_kernel(
    sizes,
    slots,
    room,
    shift_hbm,
    target_hbm,
    velocity_hbm,
    cell_hbm,
    rotation_hbm,
    axis_hbm,
    base_ref,
    code_ref,
    table_ref,
    pull_ref,
    shift_ref,
    target_ref,
    velocity_ref,
    cell_ref,
    rotation_ref,
    axis_ref,
    recv_ref,
    send_ref,
    total_ref,
    tile_ref,
    halo_ref,
    block_ref,
    plane_ref,
    kind_ref,
    direction_ref,
    load_sem,
    send_sem,
    recv_sem,
    halo_send_sem,
    halo_recv_sem,
    near_sem,
    far_sem,
):
    nx, ny, nz = sizes
    devices = nx * ny * nz
    blocks = velocity_ref.shape[1]
    per = 4 * room
    place = tuple(lax.axis_index(axis) for axis in AXES)
    me = (place[0] * ny + place[1]) * nz + place[2]

    loads = [
        pltpu.make_async_copy(source, sink, load_sem.at[i])
        for i, (source, sink) in enumerate(
            (
                (target_hbm, target_ref),
                (cell_hbm, cell_ref),
                (velocity_hbm, velocity_ref),
                (shift_hbm, shift_ref),
                (rotation_hbm, rotation_ref),
                (axis_hbm, axis_ref),
            )
        )
    ]
    for load in loads:
        load.start()

    def wrap(value, size):
        return jnp.where(value >= size, value - size, value)

    plane = nx * nz
    in_line = ny == 4
    inner_plane = (place[1] == 1) | (place[1] == 2)
    if in_line:
        buddy = jnp.where(place[1] % 2 == 0, place[1] + 1, place[1] - 1)
        upper_half = place[1] >= 2
        across = [jnp.where(upper_half, 1, 2), jnp.where(upper_half, 0, 3)]

    def number_of(there):
        return (there[0] * ny + there[1]) * nz + there[2]

    def partner(k, sign):
        stage, ox, oz = k // plane, k // nz % nx, k % nz
        if sign < 0:
            ox, oz = nx - ox, nz - oz
        if in_line:
            rows = [place[1], buddy, *across]
            if isinstance(stage, int):
                row = rows[stage]
            else:
                row = jnp.where(
                    stage < 2,
                    jnp.where(stage < 1, rows[0], rows[1]),
                    jnp.where(stage < 3, rows[2], rows[3]),
                )
        else:
            row = wrap(place[1] + (ny - stage if sign < 0 else stage), ny)
        return wrap(place[0] + ox, nx), row, wrap(place[2] + oz, nz)

    barrier = pltpu.get_barrier_semaphore()

    def greet(steps):
        for k in steps:
            pl.semaphore_signal(
                barrier, inc=1, device_id=partner(k, 1), device_id_type=MESH_ID
            )

    if in_line:
        greet(range(1, 2 * plane))

        @pl.when(inner_plane)
        def greet_across():
            greet(range(2 * plane, 3 * plane))

    else:
        greet(range(1, devices))

    loads[0].wait()
    target = target_ref[...]
    named = (lax.broadcasted_iota(jnp.int32, (devices, blocks), 0) == target).astype(jnp.float32)
    earlier = (
        lax.broadcasted_iota(jnp.int32, (blocks, blocks), 0)
        < lax.broadcasted_iota(jnp.int32, (blocks, blocks), 1)
    ).astype(jnp.float32)
    before = jnp.dot(
        named.astype(jnp.bfloat16), earlier.astype(jnp.bfloat16), preferred_element_type=jnp.float32
    )
    rank = jnp.sum(named * before, axis=0, keepdims=True).astype(jnp.int32)
    slot = target * room + rank
    chosen = (
        (lax.broadcasted_iota(jnp.int32, (devices * room, blocks), 0) == slot)
        .astype(jnp.float32)
        .astype(jnp.bfloat16)
    )
    loads[1].wait()
    codes = position_codes(cell_ref[...]).astype(jnp.float32)
    loads[2].wait()
    for channel in range(4):
        left = codes if channel == 0 else velocity_ref[channel - 1]
        placed = None
        for part in range(3):
            upper = left.astype(jnp.bfloat16)
            moved = jnp.dot(chosen, upper, preferred_element_type=jnp.float32)
            placed = moved if placed is None else placed + moved
            left = left - upper.astype(jnp.float32)
        send_ref[pl.ds(channel, devices * room, stride=4), :] = placed

    for load in loads[3:]:
        load.wait()
    lane = lax.broadcasted_iota(jnp.int32, (APER, 128), 1)
    depth_index = (lane + place[2] * CZ + shift_ref[2]) % APER
    for ex in range(CX + 1):
        index_x = ((place[0] * CX + ex) % (CX * nx) + shift_ref[0]) % APER
        layer = rotation_ref[index_x].astype(jnp.float32)
        layer = jnp.concatenate([layer] * (128 // APER), axis=1)
        block_ref[ex * APER : (ex + 1) * APER, :] = take_lanes(layer, depth_index)
        for ey in range(EY):
            index_y = ((place[1] * CY + ey) % (CY * ny) + shift_ref[1]) % APER
            row = block_ref[pl.ds(ex * APER + index_y, 1), :]
            plane_ref[ex * EY + ey : ex * EY + ey + 1, :] = row
            at = row_of_plane(ex, ey)
            kind_ref[at : at + 1, :] = row
    planes = plane_ref[0 : 8 * (PLANES // 8 + 1), :]
    sublane = lax.broadcasted_iota(jnp.int32, planes.shape, 0)
    lanes = lax.broadcasted_iota(jnp.int32, planes.shape, 1)
    first = take_lanes(planes, jnp.zeros(planes.shape, jnp.int32))
    rim_kind = jnp.sum(
        jnp.where((sublane == lanes) & (sublane < PLANES), first, 0.0), axis=0, keepdims=True
    )
    kind_ref[2 * RIM : 2 * RIM + 1, :] = rim_kind
    kind_ref[2 * RIM + 1 : 2 * RIM + 2, :] = rim_kind
    kind_ref[ROWS : 2 * TILES, :] = jnp.zeros((2 * TILES - ROWS, 128), jnp.float32)
    kinds = kind_ref[...].astype(jnp.int32)
    for component in range(3):
        direction_ref[component] = take_lanes(
            jnp.broadcast_to(axis_ref[component : component + 1, :], kinds.shape), kinds
        )

    def outgoing(k):
        there = partner(k, 1)
        number = number_of(there)
        return pltpu.make_async_remote_copy(
            src_ref=send_ref.at[pl.ds(pl.multiple_of(number * per, 8), per), :],
            dst_ref=recv_ref.at[pl.ds(pl.multiple_of(me * per, 8), per), :],
            send_sem=send_sem.at[number],
            recv_sem=recv_sem.at[me],
            device_id=there,
            device_id_type=MESH_ID,
        )

    def start(steps):
        for k in steps:
            outgoing(k).start()

    if in_line:
        pl.semaphore_wait(barrier, 2 * plane - 1 + jnp.where(inner_plane, plane, 0))

        def tell(semaphore, row):
            there = (place[0], row, place[2])
            pl.semaphore_signal(semaphore, inc=1, device_id=there, device_id_type=MESH_ID)

        @pl.when(inner_plane)
        def pass_on():
            tell(near_sem, across[0])
            tell(near_sem, buddy)

        start(range(1, 2 * plane))

        @pl.when(jnp.logical_not(inner_plane))
        def outer_hears():
            pl.semaphore_wait(near_sem, 1)

        start(range(2 * plane, 3 * plane))

        @pl.when(inner_plane)
        def inner_hears():
            pl.semaphore_wait(near_sem, 1)
            tell(far_sem, buddy)

        @pl.when(jnp.logical_not(inner_plane))
        def outer_hears_again():
            pl.semaphore_wait(far_sem, 1)

        start(range(3 * plane, devices))
    else:
        pl.semaphore_wait(barrier, devices - 1)
        start(range(1, devices))
    own = pl.ds(pl.multiple_of(me * per, 8), per)
    recv_ref[own, :] = send_ref[own, :]
    total_ref[...] = jnp.zeros(total_ref.shape, jnp.float32)
    half = lax.broadcasted_iota(jnp.int32, (8, 128), 0)

    def select_rows(source, rows, row, lane, channels, start):
        found = [jnp.zeros(row.shape, jnp.float32) for c in range(channels)]
        for r in rows:
            here = row == r
            for c in range(channels):
                at = start(r, c)
                line = jnp.broadcast_to(source[at : at + 1, :], row.shape)
                found[c] = jnp.where(here, take_lanes(line, lane), found[c])
        return found

    firsts = [0] if room <= 8 else [*range(0, room - 7, 8)] + ([room - 8] if room % 8 else [])

    def add_sender(k, part):
        base = pl.multiple_of(number_of(partner(k, -1)) * per, 8)
        by_row = lax.broadcasted_iota(jnp.int32, (8 * TILES, 128), 0) >> 3
        by_column = lax.broadcasted_iota(jnp.int32, (WIDE, 128), 0)
        lefts, rights = [], []
        for pair in range(room // 2):
            data = recv_ref[pl.ds(base + 8 * pair, 8), :]
            upper = data.astype(jnp.bfloat16).astype(jnp.float32)
            lower = data - upper
            whole = data.astype(jnp.int32)
            for which in range(2):
                if which == 0:
                    values = jnp.where(half < 4, upper, pltpu.roll(lower, 4, 0))
                else:
                    values = jnp.where(half < 4, pltpu.roll(upper, 4, 0), lower)
                values = jnp.where(half == 0, 1.0, jnp.where(half == 4, 0.0, values))
                code = whole[4 * which : 4 * which + 1]
                tiled = jnp.concatenate([values] * TILES, axis=0)
                lefts.append(jnp.where(by_row == code >> 8, tiled, 0.0).astype(jnp.bfloat16))
                rights.append(
                    (by_column == (code & (WIDE - 1))).astype(jnp.float32).astype(jnp.bfloat16)
                )
        total_ref[part] += lax.dot_general(
            jnp.concatenate(lefts, axis=1),
            jnp.concatenate(rights, axis=1),
            (((1,), (1,)), ((), ())),
            preferred_element_type=jnp.float32,
        )

    def turn_sender(k):
        number = number_of(partner(k, -1))
        base = pl.multiple_of(number * per, 8)

        for first in firsts:
            take = min(8, room)

            def rows_of(channel):
                rows = recv_ref[pl.ds(base + 4 * first + channel, take, stride=4), :]
                return jnp.concatenate([rows] * (8 // take), axis=0)

            code = rows_of(0).astype(jnp.int32)
            kind = select_rows(kind_ref, range(ROWS), code >> 7, code & 127, 1, lambda r, c: r)[0]
            kind = kind.astype(jnp.int32)
            direction = [
                take_lanes(jnp.broadcast_to(axis_ref[c : c + 1, :], (8, 128)), kind)
                for c in range(3)
            ]
            turned = rotate_about(direction, [rows_of(c + 1) for c in range(3)])
            code_ref[pl.ds(first * devices + number, take, stride=devices), :] = code[:take]
            for c in range(3):
                at = (3 * first + c) * devices + number
                base_ref[pl.ds(at, take, stride=3 * devices), :] = turned[c][:take]

    def arrived(k):
        number = number_of(partner(k, -1))
        landing = recv_ref.at[pl.ds(pl.multiple_of(number * per, 8), per), :]
        pltpu.make_async_remote_copy(
            src_ref=landing,
            dst_ref=landing,
            send_sem=send_sem.at[number],
            recv_sem=recv_sem.at[number],
            device_id=place,
            device_id_type=MESH_ID,
        ).wait_recv()

    def add_two(i, carry):
        @pl.when(i > 0)
        def first_arrived():
            arrived(2 * i)

        arrived(2 * i + 1)
        for part in range(2):
            add_sender(2 * i + part, part)
        for part in range(2):
            turn_sender(2 * i + part)
        return carry

    lax.fori_loop(0, devices // 2, add_two, 0)

    for tile in range(TILES):
        rows = pl.ds(8 * tile, 8)
        value = total_ref[0, rows, :] + total_ref[1, rows, :]
        value = value + pltpu.roll(value, 4, 0)
        tile_ref[tile] = jnp.where(half < 4, value[:, :CZ], value[:, CZ:])

    steps = neighbours(sizes)

    def slot_of(step):
        return steps.index(
            tuple(abs(d) if size == 2 else d for d, size in zip(step, sizes))
        )

    copies = []
    for step in steps:
        low, high = halo_tiles(step)
        there = tuple(
            wrap(p + d % size, size) if d else p for p, d, size in zip(place, step, sizes)
        )
        landing = slot_of(tuple(-d for d in step))
        copies.append(
            pltpu.make_async_remote_copy(
                src_ref=tile_ref.at[low:high],
                dst_ref=halo_ref.at[landing, 0 : high - low],
                send_sem=halo_send_sem.at[slot_of(step)],
                recv_sem=halo_recv_sem.at[landing],
                device_id=there,
                device_id_type=MESH_ID,
            )
        )
    for copy in copies:
        copy.start()

    def both(low, high):
        return jnp.where(half < 4, low, high)

    def finish(tile, value):
        count = both(
            jnp.broadcast_to(value[0:1], (8, 128)), jnp.broadcast_to(value[4:5], (8, 128))
        )
        table_ref[8 * tile : 8 * tile + 8, :] = value / jnp.maximum(count, 1.0)

    def pulls(low, high):
        mean = [table_ref[pl.ds(4 * low + 1 + c, high - low, stride=4), :] for c in range(3)]
        direction = [direction_ref[c, low:high, :] for c in range(3)]
        turned = rotate_about(direction, mean)
        for c in range(3):
            pull_ref[pl.ds(4 * low + 1 + c, high - low, stride=4), :] = mean[c] - turned[c]

    for tile in range(INNER, TILES):
        finish(tile, tile_ref[tile])
    pulls(BOUND, 2 * TILES)
    groups = devices // 8

    def inner(s, carry):
        for g in range(groups):
            at = pl.multiple_of(s * devices, 8) + 8 * g
            code = code_ref[pl.ds(at, 8), :]
            found = select_rows(
                pull_ref, range(BOUND, ROWS), code >> 7, code & 127, 3, lambda r, c: 4 * r + 1 + c
            )
            for c in range(3):
                place_at = pl.ds(pl.multiple_of((3 * s + c) * devices, 8) + 8 * g, 8)
                base_ref[place_at, :] = base_ref[place_at, :] + found[c]
        return carry

    lax.fori_loop(0, slots, inner, 0)

    for k in range(1, devices):
        outgoing(k).wait_send()
    for copy in copies:
        copy.wait()

    def got(step, tile):
        low, high = halo_tiles(step)
        return halo_ref[slot_of(step), tile - low]

    def turned(step, tile):
        return pltpu.roll(got(step, tile), 4, 0)

    lane = lax.broadcasted_iota(jnp.int32, (8, 128), 1)
    plane_x = (lane * 57) >> 9
    plane_y = lane - plane_x * EY

    def rim(dx, dy):
        own_rim = tile_ref[RIM] if (dx, dy) == (0, 0) else got((dx, dy, 0), RIM)
        return own_rim + both(turned((dx, dy, 1), RIM), turned((dx, dy, -1), RIM))

    for tile in range(INNER):
        value = tile_ref[tile]
        if tile < RIM or tile in (LOW, HIGH):
            value = value + both(turned((-1, 0, 0), tile), turned((1, 0, 0), tile))
        if tile in (LOW, HIGH):
            dy, other = (-1, HIGH) if tile == LOW else (1, LOW)
            value = value + got((0, dy, 0), other)
            value = value + both(turned((-1, dy, 0), other), turned((1, dy, 0), other))
        if SIDE <= tile < INNER:
            value = value + both(turned((0, -1, 0), tile), turned((0, 1, 0), tile))
        if tile == RIM:
            value = rim(0, 0)
            for dx in (-1, 0, 1):
                for dy in (-1, 0, 1):
                    if (dx, dy) == (0, 0):
                        continue
                    inside = lane < PLANES
                    if dx != 0:
                        inside = inside & (plane_x == (CX if dx > 0 else 0))
                    if dy != 0:
                        inside = inside & (plane_y == (CY if dy > 0 else 0))
                    moved = pltpu.roll(rim(dx, dy), (dx * CX * EY + dy * CY) % 128, 1)
                    value = value + jnp.where(inside, moved, 0.0)
        finish(tile, value)
    pulls(0, BOUND)


def update_kernel(slots, base_ref, code_ref, table_ref, pull_ref, out_ref, flow_ref):
    devices = out_ref.shape[2]
    sublane = lax.broadcasted_iota(jnp.int32, (CY, 128), 0)
    lane = lax.broadcasted_iota(jnp.int32, (CY, 128), 1)
    for component in range(3):
        rim = table_ref[8 * RIM + 5 + component : 8 * RIM + 6 + component, :]
        rim = jnp.broadcast_to(rim, (CY, 128))
        for ex in range(CX):
            rows = []
            for ey in range(CY):
                at = 4 * row_of_plane(ex, ey) + 1 + component
                rows.append(table_ref[at : at + 1, :])
            flow = jnp.concatenate(rows, axis=0)
            edge = take_lanes(rim, sublane + ex * EY)
            flow_ref[component, ex] = jnp.where(lane == 0, edge, flow)

    def outer(s, carry):
        for g in range(devices // 8):
            code = code_ref[pl.ds(pl.multiple_of(s * devices, 8) + 8 * g, 8), :]
            row, depth = code >> 7, code & 127
            found = [jnp.zeros((8, 128), jnp.float32) for c in range(3)]
            for r in range(BOUND):
                here = row == r
                for c in range(3):
                    at = 4 * r + 1 + c
                    line = jnp.broadcast_to(pull_ref[at : at + 1, :], (8, 128))
                    found[c] = jnp.where(here, take_lanes(line, depth), found[c])
            for c in range(3):
                at = pl.multiple_of((3 * s + c) * devices, 8) + 8 * g
                out_ref[s, c, 8 * g : 8 * g + 8, :] = base_ref[pl.ds(at, 8), :] + found[c]
        return carry

    lax.fori_loop(0, slots, outer, 0)


def shards(velocity, cell_index, block_target, rotation_axis, grid_shift):
    sizes = tuple(lax.axis_size(axis) for axis in AXES)
    devices = sizes[0] * sizes[1] * sizes[2]
    blocks = velocity.shape[0]
    lanes = velocity.shape[2]
    slots = 3 * blocks // (2 * devices)
    room = slots + slots % 2
    count = len(neighbours(sizes))
    vmem = pl.BlockSpec(memory_space=pltpu.VMEM)
    hbm = pl.BlockSpec(memory_space=pltpu.HBM)
    handed = pl.pallas_call(
        functools.partial(exchange_kernel, sizes, slots, room),
        out_shape=[
            pltpu.VMEM((room * 3 * devices, lanes), jnp.float32),
            pltpu.VMEM((room * devices, lanes), jnp.int32),
            pltpu.VMEM((8 * TILES, lanes), jnp.float32),
            pltpu.VMEM((8 * TILES, lanes), jnp.float32),
        ],
        in_specs=[hbm] * 6,
        out_specs=[vmem] * 4,
        scratch_shapes=[
            pltpu.SMEM((3,), jnp.int32),
            pltpu.VMEM((1, blocks), jnp.int32),
            pltpu.VMEM((3, blocks, lanes), jnp.float32),
            pltpu.VMEM((blocks, lanes), jnp.int32),
            pltpu.VMEM((APER, APER, APER), jnp.int32),
            pltpu.VMEM((8, 128), jnp.float32),
            pltpu.VMEM((devices * room * 4, lanes), jnp.float32),
            pltpu.VMEM((devices * room * 4, lanes), jnp.float32),
            pltpu.VMEM((2, 8 * TILES, WIDE), jnp.float32),
            pltpu.VMEM((TILES, 8, lanes), jnp.float32),
            pltpu.VMEM((count, SIDE, 8, lanes), jnp.float32),
            pltpu.VMEM(((CX + 1) * APER, lanes), jnp.float32),
            pltpu.VMEM((8 * (PLANES // 8 + 1), lanes), jnp.float32),
            pltpu.VMEM((2 * TILES, lanes), jnp.float32),
            pltpu.VMEM((3, 2 * TILES, lanes), jnp.float32),
            pltpu.SemaphoreType.DMA((6,)),
            pltpu.SemaphoreType.DMA((devices,)),
            pltpu.SemaphoreType.DMA((devices,)),
            pltpu.SemaphoreType.DMA((count,)),
            pltpu.SemaphoreType.DMA((count,)),
            pltpu.SemaphoreType.REGULAR,
            pltpu.SemaphoreType.REGULAR,
        ],
        compiler_params=pltpu.CompilerParams(collective_id=0, has_side_effects=True),
        cost_estimate=pl.CostEstimate(flops=1 << 33, bytes_accessed=1 << 21, transcendentals=0),
    )(
        grid_shift,
        block_target.reshape(1, blocks),
        jnp.transpose(velocity, (1, 0, 2)),
        cell_index,
        rotation_axis,
        jnp.asarray(axis_rows()),
    )
    updated, flow = pl.pallas_call(
        functools.partial(update_kernel, slots),
        out_shape=[
            jax.ShapeDtypeStruct((slots, 3, devices, lanes), jnp.float32),
            jax.ShapeDtypeStruct((3, CX, CY, CZ), jnp.float32),
        ],
        in_specs=[vmem] * 4,
        out_specs=[vmem, vmem],
        cost_estimate=pl.CostEstimate(flops=1 << 33, bytes_accessed=1 << 21, transcendentals=0),
    )(*[pltpu.with_memory_space_constraint(array, pltpu.VMEM) for array in handed])
    return (jnp.transpose(updated, (2, 0, 1, 3))[None], flow)


def solution(mesh):
    return jax.shard_map(
        shards,
        mesh=mesh,
        in_specs=(
            P(AXES, None, None),
            P(AXES, None),
            P(AXES, None),
            P(),
            P(),
        ),
        out_specs=(P(AXES, None, None, None, None), P(None, "gx", "gy", "gz")),
        check_vma=False,
    )
```

```python
import functools
import jax
import jax.numpy as jnp
import numpy as np
from jax import lax
from jax.experimental import pallas as pl
from jax.experimental.pallas import tpu as pltpu
from jax.sharding import PartitionSpec as P

CX = 4
CY = 8
CZ = 128
NAX = 64
APER = 32
EY = CY + 1
PLANES = (CX + 1) * EY
AXES = ("gx", "gy", "gz")
MESH_ID = pl.DeviceIdType.MESH

RIM = CY - 1
LOW = RIM + 1
HIGH = RIM + 2
SIDE = RIM + 3
INNER = SIDE + CX - 1
TILES = INNER + ((CX - 1) * (CY - 1) + 1) // 2
WIDE = 2 * CZ
BOUND = 2 * INNER
ROWS = BOUND + (CX - 1) * (CY - 1)
AHEAD = 2
SHARE = 4

angle_cosine = -0.6427876096865393
angle_sine = 0.766044443118978


def axis_rows():
    counter = np.arange(NAX) + 0.5
    height = 1.0 - 2.0 * counter / NAX
    radius = np.sqrt(np.maximum(1.0 - height * height, 0.0))
    turning = counter * 2.399963229728653
    rows = np.zeros((8, 128), np.float32)
    rows[0, :NAX] = radius * np.cos(turning)
    rows[1, :NAX] = radius * np.sin(turning)
    rows[2, :NAX] = height
    return rows


def rotate_about(direction, relative):
    inner_product = (
        direction[0] * relative[0] + direction[1] * relative[1] + direction[2] * relative[2]
    )
    crossed = [
        direction[1] * relative[2] - direction[2] * relative[1],
        direction[2] * relative[0] - direction[0] * relative[2],
        direction[0] * relative[1] - direction[1] * relative[0],
    ]
    return [
        relative[component] * angle_cosine
        + crossed[component] * angle_sine
        + direction[component] * inner_product * (1.0 - angle_cosine)
        for component in range(3)
    ]


def take_lanes(values, index):
    return jnp.take_along_axis(values, index, axis=1, mode="promise_in_bounds")


def row_of_plane(ex, ey):
    static = isinstance(ex, int)
    where = (lambda c, a, b: a if c else b) if static else jnp.where
    inner = 2 * INNER + (ex - 1) * (CY - 1) + ey - 1
    last_x = ex == CX
    last_y = ey == CY
    half_x = where(last_x, 1, 0)
    half_y = where(last_y, 1, 0)
    corner = 2 * (LOW + half_y) + half_x
    side_x = 2 * (ey - 1) + half_x
    side_y = 2 * (SIDE + ex - 1) + half_y
    edge_x = (ex == 0) | last_x
    edge_y = (ey == 0) | last_y
    return where(
        edge_x, where(edge_y, corner, side_x), where(edge_y, side_y, inner)
    )


def position_codes(cell):
    plane = (cell * 8129) >> 20
    depth = cell - plane * (CZ + 1)
    ex = (plane * 57) >> 9
    ey = plane - ex * EY
    main = row_of_plane(ex, ey) * 128 + depth
    rim = 2 * RIM * 128 + plane
    return jnp.where(depth == CZ, rim, jnp.where(depth == 0, rim + 128, main))


def neighbours(sizes):
    steps = [(0, 1) if size == 2 else (0, 1, -1) for size in sizes]
    return [
        (dx, dy, dz)
        for dx in steps[0]
        for dy in steps[1]
        for dz in steps[2]
        if (dx, dy, dz) != (0, 0, 0)
    ]


def halo_tiles(step):
    if step[2] != 0:
        return RIM, LOW
    if step[0] != 0:
        return (RIM, SIDE) if step[1] != 0 else (0, SIDE)
    return RIM, INNER


def exchange_kernel(
    sizes,
    slots,
    room,
    shift_hbm,
    target_hbm,
    velocity_hbm,
    cell_hbm,
    rotation_hbm,
    axis_hbm,
    base_ref,
    code_ref,
    table_ref,
    pull_ref,
    shift_ref,
    target_ref,
    velocity_ref,
    cell_ref,
    rotation_ref,
    axis_ref,
    recv_ref,
    send_ref,
    total_ref,
    tile_ref,
    halo_ref,
    block_ref,
    plane_ref,
    kind_ref,
    direction_ref,
    held_ref,
    load_sem,
    send_sem,
    recv_sem,
    halo_send_sem,
    halo_recv_sem,
    near_sem,
    far_sem,
):
    nx, ny, nz = sizes
    devices = nx * ny * nz
    blocks = velocity_ref.shape[1]
    per = 4 * room
    place = tuple(lax.axis_index(axis) for axis in AXES)
    me = (place[0] * ny + place[1]) * nz + place[2]

    loads = [
        pltpu.make_async_copy(source, sink, load_sem.at[i])
        for i, (source, sink) in enumerate(
            (
                (target_hbm, target_ref),
                (cell_hbm, cell_ref),
                (velocity_hbm, velocity_ref),
                (shift_hbm, shift_ref),
                (rotation_hbm, rotation_ref),
                (axis_hbm, axis_ref),
            )
        )
    ]
    for load in loads:
        load.start()

    def wrap(value, size):
        return jnp.where(value >= size, value - size, value)

    plane = nx * nz
    in_line = ny == 4
    inner_plane = (place[1] == 1) | (place[1] == 2)
    if in_line:
        buddy = jnp.where(place[1] % 2 == 0, place[1] + 1, place[1] - 1)
        upper_half = place[1] >= 2
        across = [jnp.where(upper_half, 1, 2), jnp.where(upper_half, 0, 3)]

    def number_of(there):
        return (there[0] * ny + there[1]) * nz + there[2]

    def partner(k, sign):
        stage, ox, oz = k // plane, k // nz % nx, k % nz
        if sign < 0:
            ox, oz = nx - ox, nz - oz
        if in_line:
            rows = [place[1], buddy, *across]
            if isinstance(stage, int):
                row = rows[stage]
            else:
                row = jnp.where(
                    stage < 2,
                    jnp.where(stage < 1, rows[0], rows[1]),
                    jnp.where(stage < 3, rows[2], rows[3]),
                )
        else:
            row = wrap(place[1] + (ny - stage if sign < 0 else stage), ny)
        return wrap(place[0] + ox, nx), row, wrap(place[2] + oz, nz)

    barrier = pltpu.get_barrier_semaphore()

    def greet(steps):
        for k in steps:
            pl.semaphore_signal(
                barrier, inc=1, device_id=partner(k, 1), device_id_type=MESH_ID
            )

    if in_line:
        greet(range(1, 2 * plane))

        @pl.when(inner_plane)
        def greet_across():
            greet(range(2 * plane, 3 * plane))

    else:
        greet(range(1, devices))

    for load in loads[:3]:
        load.wait()
    target = target_ref[...]
    named = (lax.broadcasted_iota(jnp.int32, (devices, blocks), 0) == target).astype(jnp.float32)
    earlier = (
        lax.broadcasted_iota(jnp.int32, (blocks, blocks), 0)
        < lax.broadcasted_iota(jnp.int32, (blocks, blocks), 1)
    ).astype(jnp.float32)
    before = jnp.dot(
        named.astype(jnp.bfloat16), earlier.astype(jnp.bfloat16), preferred_element_type=jnp.float32
    )
    rank = jnp.sum(named * before, axis=0, keepdims=True).astype(jnp.int32)
    slot = target * room + rank
    chosen = (
        (lax.broadcasted_iota(jnp.int32, (devices * room, blocks), 0) == slot)
        .astype(jnp.float32)
        .astype(jnp.bfloat16)
    )
    codes = position_codes(cell_ref[...]).astype(jnp.float32)
    lanes = codes.shape[1]
    for channel, pair in ((2, (1, 2)), (0, (None, 0))):
        left = jnp.concatenate([codes if c is None else velocity_ref[c] for c in pair], axis=1)
        placed = None
        for part in range(3):
            upper = left.astype(jnp.bfloat16)
            moved = jnp.dot(chosen, upper, preferred_element_type=jnp.float32)
            placed = moved if placed is None else placed + moved
            left = left - upper.astype(jnp.float32)
        send_ref[pl.ds(channel, devices * room, stride=4), :] = placed[:, :lanes]
        send_ref[pl.ds(channel + 1, devices * room, stride=4), :] = placed[:, lanes:]

    def outgoing(k):
        there = partner(k, 1)
        number = number_of(there)
        return pltpu.make_async_remote_copy(
            src_ref=send_ref.at[pl.ds(pl.multiple_of(number * per, 8), per), :],
            dst_ref=recv_ref.at[pl.ds(pl.multiple_of(me * per, 8), per), :],
            send_sem=send_sem.at[number],
            recv_sem=recv_sem.at[me],
            device_id=there,
            device_id_type=MESH_ID,
        )

    def start(steps):
        for k in steps:
            outgoing(k).start()

    if in_line:
        pl.semaphore_wait(barrier, 2 * plane - 1 + jnp.where(inner_plane, plane, 0))

        def tell(semaphore, row):
            there = (place[0], row, place[2])
            pl.semaphore_signal(semaphore, inc=1, device_id=there, device_id_type=MESH_ID)

        @pl.when(inner_plane)
        def pass_on():
            tell(near_sem, across[0])
            tell(near_sem, buddy)

        start(range(1, 2 * plane))

        @pl.when(jnp.logical_not(inner_plane))
        def outer_hears():
            pl.semaphore_wait(near_sem, 1)

        start(range(2 * plane, 2 * plane + AHEAD))

        @pl.when(inner_plane)
        def inner_hears():
            pl.semaphore_wait(near_sem, 1)
            tell(far_sem, buddy)

        @pl.when(jnp.logical_not(inner_plane))
        def outer_hears_again():
            pl.semaphore_wait(far_sem, 1)

        start(range(3 * plane, 3 * plane + AHEAD))
    else:
        pl.semaphore_wait(barrier, devices - 1)
        start(range(1, devices))

    for load in loads[3:]:
        load.wait()
    lane = lax.broadcasted_iota(jnp.int32, (APER, 128), 1)
    depth_index = (lane + place[2] * CZ + shift_ref[2]) % APER
    for ex in range(CX + 1):
        index_x = ((place[0] * CX + ex) % (CX * nx) + shift_ref[0]) % APER
        layer = rotation_ref[index_x].astype(jnp.float32)
        layer = jnp.concatenate([layer] * (128 // APER), axis=1)
        block_ref[ex * APER : (ex + 1) * APER, :] = take_lanes(layer, depth_index)
        for ey in range(EY):
            index_y = ((place[1] * CY + ey) % (CY * ny) + shift_ref[1]) % APER
            row = block_ref[pl.ds(ex * APER + index_y, 1), :]
            plane_ref[ex * EY + ey : ex * EY + ey + 1, :] = row
            at = row_of_plane(ex, ey)
            kind_ref[at : at + 1, :] = row
    planes = plane_ref[0 : 8 * (PLANES // 8 + 1), :]
    sublane = lax.broadcasted_iota(jnp.int32, planes.shape, 0)
    lanes = lax.broadcasted_iota(jnp.int32, planes.shape, 1)
    first = take_lanes(planes, jnp.zeros(planes.shape, jnp.int32))
    rim_kind = jnp.sum(
        jnp.where((sublane == lanes) & (sublane < PLANES), first, 0.0), axis=0, keepdims=True
    )
    kind_ref[2 * RIM : 2 * RIM + 1, :] = rim_kind
    kind_ref[2 * RIM + 1 : 2 * RIM + 2, :] = rim_kind
    kind_ref[ROWS : 2 * TILES, :] = jnp.zeros((2 * TILES - ROWS, 128), jnp.float32)
    kinds = kind_ref[...].astype(jnp.int32)
    for component in range(3):
        direction_ref[component] = take_lanes(
            jnp.broadcast_to(axis_ref[component : component + 1, :], kinds.shape), kinds
        )

    own = pl.ds(pl.multiple_of(me * per, 8), per)
    recv_ref[own, :] = send_ref[own, :]
    total_ref[...] = jnp.zeros(total_ref.shape, jnp.float32)
    pull_ref[...] = jnp.zeros(pull_ref.shape, jnp.float32)
    half = lax.broadcasted_iota(jnp.int32, (8, 128), 0)

    def select_rows(source, rows, row, lane, channels, start):
        found = [jnp.zeros(row.shape, jnp.float32) for c in range(channels)]
        for r in rows:
            here = row == r
            for c in range(channels):
                at = start(r, c)
                line = jnp.broadcast_to(source[at : at + 1, :], row.shape)
                found[c] = jnp.where(here, take_lanes(line, lane), found[c])
        return found

    firsts = [0] if room <= 8 else [*range(0, room - 7, 8)] + ([room - 8] if room % 8 else [])

    def add_sender(k, part):
        base = pl.multiple_of(number_of(partner(k, -1)) * per, 8)
        by_row = lax.broadcasted_iota(jnp.int32, (8 * TILES, 128), 0) >> 3
        by_column = lax.broadcasted_iota(jnp.int32, (WIDE, 128), 0)
        lefts, rights = [], []
        for pair in range(room // 2):
            data = recv_ref[pl.ds(base + 8 * pair, 8), :]
            upper = data.astype(jnp.bfloat16).astype(jnp.float32)
            lower = data - upper
            whole = data.astype(jnp.int32)
            for which in range(2):
                if which == 0:
                    values = jnp.where(half < 4, upper, pltpu.roll(lower, 4, 0))
                else:
                    values = jnp.where(half < 4, pltpu.roll(upper, 4, 0), lower)
                values = jnp.where(half == 0, 1.0, jnp.where(half == 4, 0.0, values))
                code = whole[4 * which : 4 * which + 1]
                tiled = jnp.concatenate([values] * TILES, axis=0)
                lefts.append(jnp.where(by_row == code >> 8, tiled, 0.0).astype(jnp.bfloat16))
                rights.append(
                    (by_column == (code & (WIDE - 1))).astype(jnp.float32).astype(jnp.bfloat16)
                )
        total_ref[part] += lax.dot_general(
            jnp.concatenate(lefts, axis=1),
            jnp.concatenate(rights, axis=1),
            (((1,), (1,)), ((), ())),
            preferred_element_type=jnp.float32,
        )

    def turn_sender(k):
        number = number_of(partner(k, -1))
        base = pl.multiple_of(number * per, 8)

        for first in firsts:
            take = min(8, room)

            def rows_of(channel):
                rows = recv_ref[pl.ds(base + 4 * first + channel, take, stride=4), :]
                return jnp.concatenate([rows] * (8 // take), axis=0)

            code = rows_of(0).astype(jnp.int32)
            kind = select_rows(kind_ref, range(ROWS), code >> 7, code & 127, 1, lambda r, c: r)[0]
            kind = kind.astype(jnp.int32)
            direction = [
                take_lanes(jnp.broadcast_to(axis_ref[c : c + 1, :], (8, 128)), kind)
                for c in range(3)
            ]
            turned = rotate_about(direction, [rows_of(c + 1) for c in range(3)])
            code_ref[pl.ds(first * devices + number, take, stride=devices), :] = code[:take]
            for c in range(3):
                at = (3 * first + c) * devices + number
                base_ref[pl.ds(at, take, stride=3 * devices), :] = turned[c][:take]

    def arrived(k):
        number = number_of(partner(k, -1))
        landing = recv_ref.at[pl.ds(pl.multiple_of(number * per, 8), per), :]
        pltpu.make_async_remote_copy(
            src_ref=landing,
            dst_ref=landing,
            send_sem=send_sem.at[number],
            recv_sem=recv_sem.at[number],
            device_id=place,
            device_id_type=MESH_ID,
        ).wait_recv()

    def add_two(i, carry):
        pair = [2 * i, 2 * i + 1]
        if in_line:
            group = i // 2

            @pl.when((i % 2 == 0) & (group + AHEAD < plane))
            def start_more():
                for stage in (2, 3):
                    outgoing(stage * plane + group).wait_send()
                    outgoing(stage * plane + group + AHEAD).start()

            pair = [
                jnp.where(i < plane, near, far)
                for near, far in zip(pair, (plane + i, 2 * plane + i))
            ]

        @pl.when(i > 0)
        def first_arrived():
            arrived(pair[0])

        arrived(pair[1])
        for part in range(2):
            add_sender(pair[part], part)
        for part in range(2):
            turn_sender(pair[part])
        return carry

    lax.fori_loop(0, devices // 2, add_two, 0)

    for tile in range(TILES):
        rows = pl.ds(8 * tile, 8)
        value = total_ref[0, rows, :] + total_ref[1, rows, :]
        value = value + pltpu.roll(value, 4, 0)
        tile_ref[tile] = jnp.where(half < 4, value[:, :CZ], value[:, CZ:])

    steps = neighbours(sizes)

    def slot_of(step):
        return steps.index(
            tuple(abs(d) if size == 2 else d for d, size in zip(step, sizes))
        )

    copies = []
    for step in steps:
        low, high = halo_tiles(step)
        there = tuple(
            wrap(p + d % size, size) if d else p for p, d, size in zip(place, step, sizes)
        )
        landing = slot_of(tuple(-d for d in step))
        copies.append(
            pltpu.make_async_remote_copy(
                src_ref=tile_ref.at[low:high],
                dst_ref=halo_ref.at[landing, 0 : high - low],
                send_sem=halo_send_sem.at[slot_of(step)],
                recv_sem=halo_recv_sem.at[landing],
                device_id=there,
                device_id_type=MESH_ID,
            )
        )
    for copy in copies:
        copy.start()

    def both(low, high):
        return jnp.where(half < 4, low, high)

    def finish(tile, value):
        count = both(
            jnp.broadcast_to(value[0:1], (8, 128)), jnp.broadcast_to(value[4:5], (8, 128))
        )
        table_ref[8 * tile : 8 * tile + 8, :] = value / jnp.maximum(count, 1.0)

    def pulls(low, high):
        mean = [table_ref[pl.ds(4 * low + 1 + c, high - low, stride=4), :] for c in range(3)]
        direction = [direction_ref[c, low:high, :] for c in range(3)]
        turned = rotate_about(direction, mean)
        for c in range(3):
            pull_ref[pl.ds(4 * low + 1 + c, high - low, stride=4), :] = mean[c] - turned[c]

    def got(step, tile):
        low, high = halo_tiles(step)
        return halo_ref[slot_of(step), tile - low]

    def turned(step, tile):
        return pltpu.roll(got(step, tile), 4, 0)

    groups = devices // 8

    def read_by_lanes(s, low, high):
        for g in range(groups):
            at = pl.multiple_of(s * devices, 8) + 8 * g
            code = code_ref[pl.ds(at, 8), :]
            found = select_rows(
                pull_ref, range(low, high), code >> 7, code & 127, 3, lambda r, c: 4 * r + 1 + c
            )
            for c in range(3):
                there = pl.ds(pl.multiple_of((3 * s + c) * devices, 8) + 8 * g, 8)
                base_ref[there, :] = base_ref[there, :] + found[c]

    def read_by_matrix(s, first, count):
        by_row = lax.broadcasted_iota(jnp.int32, (count, 256), 0) + first
        by_column = lax.broadcasted_iota(jnp.int32, (WIDE, 256), 0)
        for g in range(groups):
            at = pl.multiple_of(s * devices, 8) + 8 * g
            code = code_ref[pl.ds(at, 8), :]
            found = [[], [], []]
            for block in range(0, 8, 2):
                label = jnp.concatenate([code[block : block + 1], code[block + 1 : block + 2]], axis=1)
                onehot = (by_column == (label & (WIDE - 1))).astype(jnp.float32).astype(jnp.bfloat16)
                read = jnp.dot(
                    held_ref[0 : 6 * count, :], onehot, preferred_element_type=jnp.float32
                )
                here = by_row == label >> 8
                for c in range(3):
                    value = read[c * count : (c + 1) * count] + read[(c + 3) * count : (c + 4) * count]
                    line = jnp.sum(jnp.where(here, value, 0.0), axis=0, keepdims=True)
                    found[c] += [line[:, :128], line[:, 128:]]
            for c in range(3):
                there = pl.ds(pl.multiple_of((3 * s + c) * devices, 8) + 8 * g, 8)
                base_ref[there, :] = base_ref[there, :] + jnp.concatenate(found[c], axis=0)

    def read_rows(low, high, first, count):
        for c in range(3):
            value = jnp.concatenate(
                [
                    pull_ref[pl.ds(8 * first + 1 + c, count, stride=8), :],
                    pull_ref[pl.ds(8 * first + 5 + c, count, stride=8), :],
                ],
                axis=1,
            )
            upper = value.astype(jnp.bfloat16)
            held_ref[c * count : (c + 1) * count, :] = upper
            held_ref[(c + 3) * count : (c + 4) * count, :] = (
                value - upper.astype(jnp.float32)
            ).astype(jnp.bfloat16)

        def step(i, carry):
            read_by_matrix(SHARE * i, first, count)
            for other in range(1, SHARE):
                read_by_lanes(SHARE * i + other, low, high)
            return carry

        lax.fori_loop(0, slots // SHARE, step, 0)
        for s in range(slots - slots % SHARE, slots):
            read_by_lanes(s, low, high)

    for tile in range(INNER, TILES):
        finish(tile, tile_ref[tile])
    pulls(BOUND, 2 * TILES)
    read_rows(BOUND, ROWS, TILES - 16, 16)
    for step, copy in zip(steps, copies):
        if step[1:] == (0, 0):
            copy.wait()
    for tile in range(RIM):
        finish(
            tile,
            tile_ref[tile] + both(turned((-1, 0, 0), tile), turned((1, 0, 0), tile)),
        )
    pulls(0, 2 * RIM)
    read_rows(0, 2 * RIM, 0, 8)
    for step, copy in zip(steps, copies):
        if step[1:] != (0, 0):
            copy.wait()
    for k in range(1, devices):
        if not (in_line and k >= 2 * plane and k % plane + AHEAD < plane):
            outgoing(k).wait_send()

    lane = lax.broadcasted_iota(jnp.int32, (8, 128), 1)
    plane_x = (lane * 57) >> 9
    plane_y = lane - plane_x * EY

    def rim(dx, dy):
        own_rim = tile_ref[RIM] if (dx, dy) == (0, 0) else got((dx, dy, 0), RIM)
        return own_rim + both(turned((dx, dy, 1), RIM), turned((dx, dy, -1), RIM))

    for tile in range(RIM, INNER):
        value = tile_ref[tile]
        if tile in (LOW, HIGH):
            value = value + both(turned((-1, 0, 0), tile), turned((1, 0, 0), tile))
        if tile in (LOW, HIGH):
            dy, other = (-1, HIGH) if tile == LOW else (1, LOW)
            value = value + got((0, dy, 0), other)
            value = value + both(turned((-1, dy, 0), other), turned((1, dy, 0), other))
        if SIDE <= tile < INNER:
            value = value + both(turned((0, -1, 0), tile), turned((0, 1, 0), tile))
        if tile == RIM:
            value = rim(0, 0)
            for dx in (-1, 0, 1):
                for dy in (-1, 0, 1):
                    if (dx, dy) == (0, 0):
                        continue
                    inside = lane < PLANES
                    if dx != 0:
                        inside = inside & (plane_x == (CX if dx > 0 else 0))
                    if dy != 0:
                        inside = inside & (plane_y == (CY if dy > 0 else 0))
                    moved = pltpu.roll(rim(dx, dy), (dx * CX * EY + dy * CY) % 128, 1)
                    value = value + jnp.where(inside, moved, 0.0)
        finish(tile, value)
    pulls(2 * RIM, BOUND)


def update_kernel(slots, base_ref, code_ref, table_ref, pull_ref, out_ref, flow_ref):
    devices = out_ref.shape[2]
    sublane = lax.broadcasted_iota(jnp.int32, (CY, 128), 0)
    lane = lax.broadcasted_iota(jnp.int32, (CY, 128), 1)
    for component in range(3):
        rim = table_ref[8 * RIM + 5 + component : 8 * RIM + 6 + component, :]
        rim = jnp.broadcast_to(rim, (CY, 128))
        for ex in range(CX):
            rows = []
            for ey in range(CY):
                at = 4 * row_of_plane(ex, ey) + 1 + component
                rows.append(table_ref[at : at + 1, :])
            flow = jnp.concatenate(rows, axis=0)
            edge = take_lanes(rim, sublane + ex * EY)
            flow_ref[component, ex] = jnp.where(lane == 0, edge, flow)

    def outer(s, carry):
        for g in range(devices // 8):
            code = code_ref[pl.ds(pl.multiple_of(s * devices, 8) + 8 * g, 8), :]
            row, depth = code >> 7, code & 127
            found = [jnp.zeros((8, 128), jnp.float32) for c in range(3)]
            for r in range(2 * RIM, BOUND):
                here = row == r
                for c in range(3):
                    at = 4 * r + 1 + c
                    line = jnp.broadcast_to(pull_ref[at : at + 1, :], (8, 128))
                    found[c] = jnp.where(here, take_lanes(line, depth), found[c])
            for c in range(3):
                at = pl.multiple_of((3 * s + c) * devices, 8) + 8 * g
                out_ref[s, c, 8 * g : 8 * g + 8, :] = base_ref[pl.ds(at, 8), :] + found[c]
        return carry

    lax.fori_loop(0, slots, outer, 0)


def shards(velocity, cell_index, block_target, rotation_axis, grid_shift):
    sizes = tuple(lax.axis_size(axis) for axis in AXES)
    devices = sizes[0] * sizes[1] * sizes[2]
    blocks = velocity.shape[0]
    lanes = velocity.shape[2]
    slots = 3 * blocks // (2 * devices)
    room = slots + slots % 2
    count = len(neighbours(sizes))
    vmem = pl.BlockSpec(memory_space=pltpu.VMEM)
    hbm = pl.BlockSpec(memory_space=pltpu.HBM)
    handed = pl.pallas_call(
        functools.partial(exchange_kernel, sizes, slots, room),
        out_shape=[
            pltpu.VMEM((room * 3 * devices, lanes), jnp.float32),
            pltpu.VMEM((room * devices, lanes), jnp.int32),
            pltpu.VMEM((8 * TILES, lanes), jnp.float32),
            pltpu.VMEM((8 * TILES, lanes), jnp.float32),
        ],
        in_specs=[hbm] * 6,
        out_specs=[vmem] * 4,
        scratch_shapes=[
            pltpu.SMEM((3,), jnp.int32),
            pltpu.VMEM((1, blocks), jnp.int32),
            pltpu.VMEM((3, blocks, lanes), jnp.float32),
            pltpu.VMEM((blocks, lanes), jnp.int32),
            pltpu.VMEM((APER, APER, APER), jnp.int32),
            pltpu.VMEM((8, 128), jnp.float32),
            pltpu.VMEM((devices * room * 4, lanes), jnp.float32),
            pltpu.VMEM((devices * room * 4, lanes), jnp.float32),
            pltpu.VMEM((2, 8 * TILES, WIDE), jnp.float32),
            pltpu.VMEM((TILES, 8, lanes), jnp.float32),
            pltpu.VMEM((count, SIDE, 8, lanes), jnp.float32),
            pltpu.VMEM(((CX + 1) * APER, lanes), jnp.float32),
            pltpu.VMEM((8 * (PLANES // 8 + 1), lanes), jnp.float32),
            pltpu.VMEM((2 * TILES, lanes), jnp.float32),
            pltpu.VMEM((3, 2 * TILES, lanes), jnp.float32),
            pltpu.VMEM((6 * 16, WIDE), jnp.bfloat16),
            pltpu.SemaphoreType.DMA((6,)),
            pltpu.SemaphoreType.DMA((devices,)),
            pltpu.SemaphoreType.DMA((devices,)),
            pltpu.SemaphoreType.DMA((count,)),
            pltpu.SemaphoreType.DMA((count,)),
            pltpu.SemaphoreType.REGULAR,
            pltpu.SemaphoreType.REGULAR,
        ],
        compiler_params=pltpu.CompilerParams(collective_id=0, has_side_effects=True),
        cost_estimate=pl.CostEstimate(flops=1 << 33, bytes_accessed=1 << 21, transcendentals=0),
    )(
        grid_shift,
        block_target.reshape(1, blocks),
        jnp.transpose(velocity, (1, 0, 2)),
        cell_index,
        rotation_axis,
        jnp.asarray(axis_rows()),
    )
    updated, flow = pl.pallas_call(
        functools.partial(update_kernel, slots),
        out_shape=[
            jax.ShapeDtypeStruct((slots, 3, devices, lanes), jnp.float32),
            jax.ShapeDtypeStruct((3, CX, CY, CZ), jnp.float32),
        ],
        in_specs=[vmem] * 4,
        out_specs=[vmem, vmem],
        cost_estimate=pl.CostEstimate(flops=1 << 33, bytes_accessed=1 << 21, transcendentals=0),
    )(*[pltpu.with_memory_space_constraint(array, pltpu.VMEM) for array in handed])
    return (jnp.transpose(updated, (2, 0, 1, 3))[None], flow)


def solution(mesh):
    return jax.shard_map(
        shards,
        mesh=mesh,
        in_specs=(
            P(AXES, None, None),
            P(AXES, None),
            P(AXES, None),
            P(),
            P(),
        ),
        out_specs=(P(AXES, None, None, None, None), P(None, "gx", "gy", "gz")),
        check_vma=False,
    )
```

```python
import functools
import jax
import jax.numpy as jnp
import numpy as np
from jax import lax
from jax.experimental import pallas as pl
from jax.experimental.pallas import tpu as pltpu
from jax.sharding import PartitionSpec as P

CX = 4
CY = 8
CZ = 128
NAX = 64
APER = 32
EY = CY + 1
PLANES = (CX + 1) * EY
AXES = ("gx", "gy", "gz")
MESH_ID = pl.DeviceIdType.MESH

RIM = CY - 1
LOW = RIM + 1
HIGH = RIM + 2
SIDE = RIM + 3
INNER = SIDE + CX - 1
TILES = INNER + ((CX - 1) * (CY - 1) + 1) // 2
WIDE = 2 * CZ
BOUND = 2 * INNER
ROWS = BOUND + (CX - 1) * (CY - 1)
AHEAD = 3
SHARE = 4

angle_cosine = -0.6427876096865393
angle_sine = 0.766044443118978


def axis_rows():
    counter = np.arange(NAX) + 0.5
    height = 1.0 - 2.0 * counter / NAX
    radius = np.sqrt(np.maximum(1.0 - height * height, 0.0))
    turning = counter * 2.399963229728653
    rows = np.zeros((8, 128), np.float32)
    rows[0, :NAX] = radius * np.cos(turning)
    rows[1, :NAX] = radius * np.sin(turning)
    rows[2, :NAX] = height
    return rows


def rotate_about(direction, relative):
    inner_product = (
        direction[0] * relative[0] + direction[1] * relative[1] + direction[2] * relative[2]
    )
    crossed = [
        direction[1] * relative[2] - direction[2] * relative[1],
        direction[2] * relative[0] - direction[0] * relative[2],
        direction[0] * relative[1] - direction[1] * relative[0],
    ]
    return [
        relative[component] * angle_cosine
        + crossed[component] * angle_sine
        + direction[component] * inner_product * (1.0 - angle_cosine)
        for component in range(3)
    ]


def take_lanes(values, index):
    return jnp.take_along_axis(values, index, axis=1, mode="promise_in_bounds")


def row_of_plane(ex, ey):
    static = isinstance(ex, int)
    where = (lambda c, a, b: a if c else b) if static else jnp.where
    inner = 2 * INNER + (ex - 1) * (CY - 1) + ey - 1
    last_x = ex == CX
    last_y = ey == CY
    half_x = where(last_x, 1, 0)
    half_y = where(last_y, 1, 0)
    corner = 2 * (LOW + half_y) + half_x
    side_x = 2 * (ey - 1) + half_x
    side_y = 2 * (SIDE + ex - 1) + half_y
    edge_x = (ex == 0) | last_x
    edge_y = (ey == 0) | last_y
    return where(
        edge_x, where(edge_y, corner, side_x), where(edge_y, side_y, inner)
    )


def position_codes(cell):
    plane = (cell * 8129) >> 20
    depth = cell - plane * (CZ + 1)
    ex = (plane * 57) >> 9
    ey = plane - ex * EY
    main = row_of_plane(ex, ey) * 128 + depth
    rim = 2 * RIM * 128 + plane
    return jnp.where(depth == CZ, rim, jnp.where(depth == 0, rim + 128, main))


def neighbours(sizes):
    steps = [(0, 1) if size == 2 else (0, 1, -1) for size in sizes]
    return [
        (dx, dy, dz)
        for dx in steps[0]
        for dy in steps[1]
        for dz in steps[2]
        if (dx, dy, dz) != (0, 0, 0)
    ]


def halo_tiles(step):
    if step[2] != 0:
        return RIM, LOW
    if step[0] != 0:
        return (RIM, SIDE) if step[1] != 0 else (0, SIDE)
    return RIM, INNER


def exchange_kernel(
    sizes,
    slots,
    room,
    shift_hbm,
    target_hbm,
    velocity_hbm,
    cell_hbm,
    rotation_hbm,
    axis_hbm,
    base_ref,
    code_ref,
    table_ref,
    pull_ref,
    shift_ref,
    target_ref,
    velocity_ref,
    cell_ref,
    rotation_ref,
    axis_ref,
    recv_ref,
    send_ref,
    total_ref,
    tile_ref,
    halo_ref,
    block_ref,
    plane_ref,
    kind_ref,
    direction_ref,
    held_ref,
    load_sem,
    send_sem,
    recv_sem,
    halo_send_sem,
    halo_recv_sem,
    near_sem,
    far_sem,
):
    nx, ny, nz = sizes
    devices = nx * ny * nz
    blocks = velocity_ref.shape[1]
    per = 4 * room
    place = tuple(lax.axis_index(axis) for axis in AXES)
    me = (place[0] * ny + place[1]) * nz + place[2]

    loads = [
        pltpu.make_async_copy(source, sink, load_sem.at[i])
        for i, (source, sink) in enumerate(
            (
                (target_hbm, target_ref),
                (cell_hbm, cell_ref),
                (velocity_hbm, velocity_ref),
                (shift_hbm, shift_ref),
                (rotation_hbm, rotation_ref),
                (axis_hbm, axis_ref),
            )
        )
    ]
    for load in loads[:3]:
        load.start()

    def wrap(value, size):
        return jnp.where(value >= size, value - size, value)

    plane = nx * nz
    in_line = ny == 4
    inner_plane = (place[1] == 1) | (place[1] == 2)
    if in_line:
        buddy = jnp.where(place[1] % 2 == 0, place[1] + 1, place[1] - 1)
        upper_half = place[1] >= 2
        across = [jnp.where(upper_half, 1, 2), jnp.where(upper_half, 0, 3)]

    def number_of(there):
        return (there[0] * ny + there[1]) * nz + there[2]

    def partner(k, sign):
        stage, ox, oz = k // plane, k // nz % nx, k % nz
        if sign < 0:
            ox, oz = nx - ox, nz - oz
        if in_line:
            rows = [place[1], buddy, *across]
            if isinstance(stage, int):
                row = rows[stage]
            else:
                row = jnp.where(
                    stage < 2,
                    jnp.where(stage < 1, rows[0], rows[1]),
                    jnp.where(stage < 3, rows[2], rows[3]),
                )
        else:
            row = wrap(place[1] + (ny - stage if sign < 0 else stage), ny)
        return wrap(place[0] + ox, nx), row, wrap(place[2] + oz, nz)

    barrier = pltpu.get_barrier_semaphore()

    def greet(steps):
        for k in steps:
            pl.semaphore_signal(
                barrier, inc=1, device_id=partner(k, 1), device_id_type=MESH_ID
            )

    if in_line:
        greet(range(1, 2 * plane))

        @pl.when(inner_plane)
        def greet_across():
            greet(range(2 * plane, 3 * plane))

    else:
        greet(range(1, devices))

    for load in loads[:3]:
        load.wait()
    for load in loads[3:]:
        load.start()
    target = target_ref[...]
    named = (lax.broadcasted_iota(jnp.int32, (devices, blocks), 0) == target).astype(jnp.float32)
    earlier = (
        lax.broadcasted_iota(jnp.int32, (blocks, blocks), 0)
        < lax.broadcasted_iota(jnp.int32, (blocks, blocks), 1)
    ).astype(jnp.float32)
    before = jnp.dot(
        named.astype(jnp.bfloat16), earlier.astype(jnp.bfloat16), preferred_element_type=jnp.float32
    )
    rank = jnp.sum(named * before, axis=0, keepdims=True).astype(jnp.int32)
    slot = target * room + rank
    chosen = (
        (lax.broadcasted_iota(jnp.int32, (devices * room, blocks), 0) == slot)
        .astype(jnp.float32)
        .astype(jnp.bfloat16)
    )
    codes = position_codes(cell_ref[...]).astype(jnp.float32)
    lanes = codes.shape[1]
    for channel, pair in ((2, (1, 2)), (0, (None, 0))):
        left = jnp.concatenate([codes if c is None else velocity_ref[c] for c in pair], axis=1)
        placed = None
        for part in range(3):
            upper = left.astype(jnp.bfloat16)
            moved = jnp.dot(chosen, upper, preferred_element_type=jnp.float32)
            placed = moved if placed is None else placed + moved
            left = left - upper.astype(jnp.float32)
        send_ref[pl.ds(channel, devices * room, stride=4), :] = placed[:, :lanes]
        send_ref[pl.ds(channel + 1, devices * room, stride=4), :] = placed[:, lanes:]

    def outgoing(k):
        there = partner(k, 1)
        number = number_of(there)
        return pltpu.make_async_remote_copy(
            src_ref=send_ref.at[pl.ds(pl.multiple_of(number * per, 8), per), :],
            dst_ref=recv_ref.at[pl.ds(pl.multiple_of(me * per, 8), per), :],
            send_sem=send_sem.at[number],
            recv_sem=recv_sem.at[me],
            device_id=there,
            device_id_type=MESH_ID,
        )

    def start(steps):
        for k in steps:
            outgoing(k).start()

    if in_line:
        pl.semaphore_wait(barrier, 2 * plane - 1 + jnp.where(inner_plane, plane, 0))

        def tell(semaphore, row):
            there = (place[0], row, place[2])
            pl.semaphore_signal(semaphore, inc=1, device_id=there, device_id_type=MESH_ID)

        @pl.when(inner_plane)
        def pass_on():
            tell(near_sem, across[0])
            tell(near_sem, buddy)

        start(range(1, 2 * plane))

        @pl.when(jnp.logical_not(inner_plane))
        def outer_hears():
            pl.semaphore_wait(near_sem, 1)

        start(range(2 * plane, 2 * plane + AHEAD))

        @pl.when(inner_plane)
        def inner_hears():
            pl.semaphore_wait(near_sem, 1)
            tell(far_sem, buddy)

        @pl.when(jnp.logical_not(inner_plane))
        def outer_hears_again():
            pl.semaphore_wait(far_sem, 1)

        start(range(3 * plane, 3 * plane + AHEAD))
    else:
        pl.semaphore_wait(barrier, devices - 1)
        start(range(1, devices))

    for load in loads[3:]:
        load.wait()
    lane = lax.broadcasted_iota(jnp.int32, (APER, 128), 1)
    depth_index = (lane + place[2] * CZ + shift_ref[2]) % APER
    for ex in range(CX + 1):
        index_x = ((place[0] * CX + ex) % (CX * nx) + shift_ref[0]) % APER
        layer = rotation_ref[index_x].astype(jnp.float32)
        layer = jnp.concatenate([layer] * (128 // APER), axis=1)
        block_ref[ex * APER : (ex + 1) * APER, :] = take_lanes(layer, depth_index)
        for ey in range(EY):
            index_y = ((place[1] * CY + ey) % (CY * ny) + shift_ref[1]) % APER
            row = block_ref[pl.ds(ex * APER + index_y, 1), :]
            plane_ref[ex * EY + ey : ex * EY + ey + 1, :] = row
            at = row_of_plane(ex, ey)
            kind_ref[at : at + 1, :] = row
    planes = plane_ref[0 : 8 * (PLANES // 8 + 1), :]
    sublane = lax.broadcasted_iota(jnp.int32, planes.shape, 0)
    lanes = lax.broadcasted_iota(jnp.int32, planes.shape, 1)
    first = take_lanes(planes, jnp.zeros(planes.shape, jnp.int32))
    rim_kind = jnp.sum(
        jnp.where((sublane == lanes) & (sublane < PLANES), first, 0.0), axis=0, keepdims=True
    )
    kind_ref[2 * RIM : 2 * RIM + 1, :] = rim_kind
    kind_ref[2 * RIM + 1 : 2 * RIM + 2, :] = rim_kind
    kind_ref[ROWS : 2 * TILES, :] = jnp.zeros((2 * TILES - ROWS, 128), jnp.float32)
    kinds = kind_ref[...].astype(jnp.int32)
    for component in range(3):
        direction_ref[component] = take_lanes(
            jnp.broadcast_to(axis_ref[component : component + 1, :], kinds.shape), kinds
        )

    own = pl.ds(pl.multiple_of(me * per, 8), per)
    recv_ref[own, :] = send_ref[own, :]
    total_ref[...] = jnp.zeros(total_ref.shape, jnp.float32)
    pull_ref[...] = jnp.zeros(pull_ref.shape, jnp.float32)
    half = lax.broadcasted_iota(jnp.int32, (8, 128), 0)

    def select_rows(source, rows, row, lane, channels, start):
        found = [jnp.zeros(row.shape, jnp.float32) for c in range(channels)]
        for r in rows:
            here = row == r
            for c in range(channels):
                at = start(r, c)
                line = jnp.broadcast_to(source[at : at + 1, :], row.shape)
                found[c] = jnp.where(here, take_lanes(line, lane), found[c])
        return found

    firsts = [0] if room <= 8 else [*range(0, room - 7, 8)] + ([room - 8] if room % 8 else [])

    def add_sender(k, part):
        base = pl.multiple_of(number_of(partner(k, -1)) * per, 8)
        by_row = lax.broadcasted_iota(jnp.int32, (8 * TILES, 128), 0) >> 3
        by_column = lax.broadcasted_iota(jnp.int32, (WIDE, 128), 0)
        lefts, rights = [], []
        for pair in range(room // 2):
            data = recv_ref[pl.ds(base + 8 * pair, 8), :]
            upper = data.astype(jnp.bfloat16).astype(jnp.float32)
            lower = data - upper
            whole = data.astype(jnp.int32)
            for which in range(2):
                if which == 0:
                    values = jnp.where(half < 4, upper, pltpu.roll(lower, 4, 0))
                else:
                    values = jnp.where(half < 4, pltpu.roll(upper, 4, 0), lower)
                values = jnp.where(half == 0, 1.0, jnp.where(half == 4, 0.0, values))
                code = whole[4 * which : 4 * which + 1]
                tiled = jnp.concatenate([values] * TILES, axis=0)
                lefts.append(jnp.where(by_row == code >> 8, tiled, 0.0).astype(jnp.bfloat16))
                rights.append(
                    (by_column == (code & (WIDE - 1))).astype(jnp.float32).astype(jnp.bfloat16)
                )
        total_ref[part] += lax.dot_general(
            jnp.concatenate(lefts, axis=1),
            jnp.concatenate(rights, axis=1),
            (((1,), (1,)), ((), ())),
            preferred_element_type=jnp.float32,
        )

    def turn_sender(k):
        number = number_of(partner(k, -1))
        base = pl.multiple_of(number * per, 8)

        for first in firsts:
            take = min(8, room)

            def rows_of(channel):
                rows = recv_ref[pl.ds(base + 4 * first + channel, take, stride=4), :]
                return jnp.concatenate([rows] * (8 // take), axis=0)

            code = rows_of(0).astype(jnp.int32)
            kind = select_rows(kind_ref, range(ROWS), code >> 7, code & 127, 1, lambda r, c: r)[0]
            kind = kind.astype(jnp.int32)
            direction = [
                take_lanes(jnp.broadcast_to(axis_ref[c : c + 1, :], (8, 128)), kind)
                for c in range(3)
            ]
            turned = rotate_about(direction, [rows_of(c + 1) for c in range(3)])
            code_ref[pl.ds(first * devices + number, take, stride=devices), :] = code[:take]
            for c in range(3):
                at = (3 * first + c) * devices + number
                base_ref[pl.ds(at, take, stride=3 * devices), :] = turned[c][:take]

    def arrived(k):
        number = number_of(partner(k, -1))
        landing = recv_ref.at[pl.ds(pl.multiple_of(number * per, 8), per), :]
        pltpu.make_async_remote_copy(
            src_ref=landing,
            dst_ref=landing,
            send_sem=send_sem.at[number],
            recv_sem=recv_sem.at[number],
            device_id=place,
            device_id_type=MESH_ID,
        ).wait_recv()

    def add_two(i, carry):
        pair = [2 * i, 2 * i + 1]
        if in_line:
            group = i // 2

            @pl.when((i % 2 == 0) & (group + AHEAD < plane))
            def start_more():
                for stage in (2, 3):
                    outgoing(stage * plane + group).wait_send()
                    outgoing(stage * plane + group + AHEAD).start()

            pair = [
                jnp.where(i < plane, near, far)
                for near, far in zip(pair, (plane + i, 2 * plane + i))
            ]

        @pl.when(i > 0)
        def first_arrived():
            arrived(pair[0])

        arrived(pair[1])
        for part in range(2):
            add_sender(pair[part], part)
        for part in range(2):
            turn_sender(pair[part])
        return carry

    lax.fori_loop(0, devices // 2, add_two, 0)

    for tile in range(TILES):
        rows = pl.ds(8 * tile, 8)
        value = total_ref[0, rows, :] + total_ref[1, rows, :]
        value = value + pltpu.roll(value, 4, 0)
        tile_ref[tile] = jnp.where(half < 4, value[:, :CZ], value[:, CZ:])

    steps = neighbours(sizes)

    def slot_of(step):
        return steps.index(
            tuple(abs(d) if size == 2 else d for d, size in zip(step, sizes))
        )

    copies = []
    for step in steps:
        low, high = halo_tiles(step)
        there = tuple(
            wrap(p + d % size, size) if d else p for p, d, size in zip(place, step, sizes)
        )
        landing = slot_of(tuple(-d for d in step))
        copies.append(
            pltpu.make_async_remote_copy(
                src_ref=tile_ref.at[low:high],
                dst_ref=halo_ref.at[landing, 0 : high - low],
                send_sem=halo_send_sem.at[slot_of(step)],
                recv_sem=halo_recv_sem.at[landing],
                device_id=there,
                device_id_type=MESH_ID,
            )
        )
    for copy in copies:
        copy.start()

    def both(low, high):
        return jnp.where(half < 4, low, high)

    def finish(tile, value):
        count = both(
            jnp.broadcast_to(value[0:1], (8, 128)), jnp.broadcast_to(value[4:5], (8, 128))
        )
        table_ref[8 * tile : 8 * tile + 8, :] = value / jnp.maximum(count, 1.0)

    def pulls(low, high):
        mean = [table_ref[pl.ds(4 * low + 1 + c, high - low, stride=4), :] for c in range(3)]
        direction = [direction_ref[c, low:high, :] for c in range(3)]
        turned = rotate_about(direction, mean)
        for c in range(3):
            pull_ref[pl.ds(4 * low + 1 + c, high - low, stride=4), :] = mean[c] - turned[c]

    def got(step, tile):
        low, high = halo_tiles(step)
        return halo_ref[slot_of(step), tile - low]

    def turned(step, tile):
        return pltpu.roll(got(step, tile), 4, 0)

    groups = devices // 8

    def read_by_lanes(s, low, high):
        for g in range(groups):
            at = pl.multiple_of(s * devices, 8) + 8 * g
            code = code_ref[pl.ds(at, 8), :]
            found = select_rows(
                pull_ref, range(low, high), code >> 7, code & 127, 3, lambda r, c: 4 * r + 1 + c
            )
            for c in range(3):
                there = pl.ds(pl.multiple_of((3 * s + c) * devices, 8) + 8 * g, 8)
                base_ref[there, :] = base_ref[there, :] + found[c]

    def read_by_matrix(s, first, count):
        by_row = lax.broadcasted_iota(jnp.int32, (count, 256), 0) + first
        by_column = lax.broadcasted_iota(jnp.int32, (WIDE, 256), 0)
        for g in range(groups):
            at = pl.multiple_of(s * devices, 8) + 8 * g
            code = code_ref[pl.ds(at, 8), :]
            found = [[], [], []]
            for block in range(0, 8, 2):
                label = jnp.concatenate([code[block : block + 1], code[block + 1 : block + 2]], axis=1)
                onehot = (by_column == (label & (WIDE - 1))).astype(jnp.float32).astype(jnp.bfloat16)
                read = jnp.dot(
                    held_ref[0 : 6 * count, :], onehot, preferred_element_type=jnp.float32
                )
                here = by_row == label >> 8
                for c in range(3):
                    value = read[c * count : (c + 1) * count] + read[(c + 3) * count : (c + 4) * count]
                    line = jnp.sum(jnp.where(here, value, 0.0), axis=0, keepdims=True)
                    found[c] += [line[:, :128], line[:, 128:]]
            for c in range(3):
                there = pl.ds(pl.multiple_of((3 * s + c) * devices, 8) + 8 * g, 8)
                base_ref[there, :] = base_ref[there, :] + jnp.concatenate(found[c], axis=0)

    def read_rows(low, high, first, count):
        for c in range(3):
            value = jnp.concatenate(
                [
                    pull_ref[pl.ds(8 * first + 1 + c, count, stride=8), :],
                    pull_ref[pl.ds(8 * first + 5 + c, count, stride=8), :],
                ],
                axis=1,
            )
            upper = value.astype(jnp.bfloat16)
            held_ref[c * count : (c + 1) * count, :] = upper
            held_ref[(c + 3) * count : (c + 4) * count, :] = (
                value - upper.astype(jnp.float32)
            ).astype(jnp.bfloat16)

        def step(i, carry):
            read_by_matrix(SHARE * i, first, count)
            for other in range(1, SHARE):
                read_by_lanes(SHARE * i + other, low, high)
            return carry

        lax.fori_loop(0, slots // SHARE, step, 0)
        for s in range(slots - slots % SHARE, slots):
            read_by_lanes(s, low, high)

    for tile in range(INNER, TILES):
        finish(tile, tile_ref[tile])
    pulls(BOUND, 2 * TILES)
    read_rows(BOUND, ROWS, TILES - 16, 16)
    for step, copy in zip(steps, copies):
        if step[1:] == (0, 0):
            copy.wait()
    for tile in range(RIM):
        finish(
            tile,
            tile_ref[tile] + both(turned((-1, 0, 0), tile), turned((1, 0, 0), tile)),
        )
    pulls(0, 2 * RIM)
    read_rows(0, 2 * RIM, 0, 8)
    for step, copy in zip(steps, copies):
        if step[1:] != (0, 0):
            copy.wait()
    for k in range(1, devices):
        if not (in_line and k >= 2 * plane and k % plane + AHEAD < plane):
            outgoing(k).wait_send()

    lane = lax.broadcasted_iota(jnp.int32, (8, 128), 1)
    plane_x = (lane * 57) >> 9
    plane_y = lane - plane_x * EY

    def rim(dx, dy):
        own_rim = tile_ref[RIM] if (dx, dy) == (0, 0) else got((dx, dy, 0), RIM)
        return own_rim + both(turned((dx, dy, 1), RIM), turned((dx, dy, -1), RIM))

    for tile in range(RIM, INNER):
        value = tile_ref[tile]
        if tile in (LOW, HIGH):
            value = value + both(turned((-1, 0, 0), tile), turned((1, 0, 0), tile))
        if tile in (LOW, HIGH):
            dy, other = (-1, HIGH) if tile == LOW else (1, LOW)
            value = value + got((0, dy, 0), other)
            value = value + both(turned((-1, dy, 0), other), turned((1, dy, 0), other))
        if SIDE <= tile < INNER:
            value = value + both(turned((0, -1, 0), tile), turned((0, 1, 0), tile))
        if tile == RIM:
            value = rim(0, 0)
            for dx in (-1, 0, 1):
                for dy in (-1, 0, 1):
                    if (dx, dy) == (0, 0):
                        continue
                    inside = lane < PLANES
                    if dx != 0:
                        inside = inside & (plane_x == (CX if dx > 0 else 0))
                    if dy != 0:
                        inside = inside & (plane_y == (CY if dy > 0 else 0))
                    moved = pltpu.roll(rim(dx, dy), (dx * CX * EY + dy * CY) % 128, 1)
                    value = value + jnp.where(inside, moved, 0.0)
        finish(tile, value)
    pulls(2 * RIM, BOUND)


def update_kernel(slots, base_ref, code_ref, table_ref, pull_ref, out_ref, flow_ref):
    devices = out_ref.shape[2]
    sublane = lax.broadcasted_iota(jnp.int32, (CY, 128), 0)
    lane = lax.broadcasted_iota(jnp.int32, (CY, 128), 1)
    for component in range(3):
        rim = table_ref[8 * RIM + 5 + component : 8 * RIM + 6 + component, :]
        rim = jnp.broadcast_to(rim, (CY, 128))
        for ex in range(CX):
            rows = []
            for ey in range(CY):
                at = 4 * row_of_plane(ex, ey) + 1 + component
                rows.append(table_ref[at : at + 1, :])
            flow = jnp.concatenate(rows, axis=0)
            edge = take_lanes(rim, sublane + ex * EY)
            flow_ref[component, ex] = jnp.where(lane == 0, edge, flow)

    def outer(s, carry):
        for g in range(devices // 8):
            code = code_ref[pl.ds(pl.multiple_of(s * devices, 8) + 8 * g, 8), :]
            row, depth = code >> 7, code & 127
            found = [jnp.zeros((8, 128), jnp.float32) for c in range(3)]
            for r in range(2 * RIM, BOUND):
                here = row == r
                for c in range(3):
                    at = 4 * r + 1 + c
                    line = jnp.broadcast_to(pull_ref[at : at + 1, :], (8, 128))
                    found[c] = jnp.where(here, take_lanes(line, depth), found[c])
            for c in range(3):
                at = pl.multiple_of((3 * s + c) * devices, 8) + 8 * g
                out_ref[s, c, 8 * g : 8 * g + 8, :] = base_ref[pl.ds(at, 8), :] + found[c]
        return carry

    lax.fori_loop(0, slots, outer, 0)


def shards(velocity, cell_index, block_target, rotation_axis, grid_shift):
    sizes = tuple(lax.axis_size(axis) for axis in AXES)
    devices = sizes[0] * sizes[1] * sizes[2]
    blocks = velocity.shape[0]
    lanes = velocity.shape[2]
    slots = 3 * blocks // (2 * devices)
    room = slots + slots % 2
    count = len(neighbours(sizes))
    vmem = pl.BlockSpec(memory_space=pltpu.VMEM)
    hbm = pl.BlockSpec(memory_space=pltpu.HBM)
    handed = pl.pallas_call(
        functools.partial(exchange_kernel, sizes, slots, room),
        out_shape=[
            pltpu.VMEM((room * 3 * devices, lanes), jnp.float32),
            pltpu.VMEM((room * devices, lanes), jnp.int32),
            pltpu.VMEM((8 * TILES, lanes), jnp.float32),
            pltpu.VMEM((8 * TILES, lanes), jnp.float32),
        ],
        in_specs=[hbm] * 6,
        out_specs=[vmem] * 4,
        scratch_shapes=[
            pltpu.SMEM((3,), jnp.int32),
            pltpu.VMEM((1, blocks), jnp.int32),
            pltpu.VMEM((3, blocks, lanes), jnp.float32),
            pltpu.VMEM((blocks, lanes), jnp.int32),
            pltpu.VMEM((APER, APER, APER), jnp.int32),
            pltpu.VMEM((8, 128), jnp.float32),
            pltpu.VMEM((devices * room * 4, lanes), jnp.float32),
            pltpu.VMEM((devices * room * 4, lanes), jnp.float32),
            pltpu.VMEM((2, 8 * TILES, WIDE), jnp.float32),
            pltpu.VMEM((TILES, 8, lanes), jnp.float32),
            pltpu.VMEM((count, SIDE, 8, lanes), jnp.float32),
            pltpu.VMEM(((CX + 1) * APER, lanes), jnp.float32),
            pltpu.VMEM((8 * (PLANES // 8 + 1), lanes), jnp.float32),
            pltpu.VMEM((2 * TILES, lanes), jnp.float32),
            pltpu.VMEM((3, 2 * TILES, lanes), jnp.float32),
            pltpu.VMEM((6 * 16, WIDE), jnp.bfloat16),
            pltpu.SemaphoreType.DMA((6,)),
            pltpu.SemaphoreType.DMA((devices,)),
            pltpu.SemaphoreType.DMA((devices,)),
            pltpu.SemaphoreType.DMA((count,)),
            pltpu.SemaphoreType.DMA((count,)),
            pltpu.SemaphoreType.REGULAR,
            pltpu.SemaphoreType.REGULAR,
        ],
        compiler_params=pltpu.CompilerParams(collective_id=0, has_side_effects=True),
        cost_estimate=pl.CostEstimate(flops=1 << 33, bytes_accessed=1 << 21, transcendentals=0),
    )(
        grid_shift,
        block_target.reshape(1, blocks),
        jnp.transpose(velocity, (1, 0, 2)),
        cell_index,
        rotation_axis,
        jnp.asarray(axis_rows()),
    )
    updated, flow = pl.pallas_call(
        functools.partial(update_kernel, slots),
        out_shape=[
            jax.ShapeDtypeStruct((slots, 3, devices, lanes), jnp.float32),
            jax.ShapeDtypeStruct((3, CX, CY, CZ), jnp.float32),
        ],
        in_specs=[vmem] * 4,
        out_specs=[vmem, vmem],
        cost_estimate=pl.CostEstimate(flops=1 << 33, bytes_accessed=1 << 21, transcendentals=0),
    )(*[pltpu.with_memory_space_constraint(array, pltpu.VMEM) for array in handed])
    return (jnp.transpose(updated, (2, 0, 1, 3))[None], flow)


def solution(mesh):
    return jax.shard_map(
        shards,
        mesh=mesh,
        in_specs=(
            P(AXES, None, None),
            P(AXES, None),
            P(AXES, None),
            P(),
            P(),
        ),
        out_specs=(P(AXES, None, None, None, None), P(None, "gx", "gy", "gz")),
        check_vma=False,
    )
```

```python
import functools
import jax
import jax.numpy as jnp
import numpy as np
from jax import lax
from jax.experimental import pallas as pl
from jax.experimental.pallas import tpu as pltpu
from jax.sharding import PartitionSpec as P

CX = 4
CY = 8
CZ = 128
NAX = 64
APER = 32
EY = CY + 1
PLANES = (CX + 1) * EY
AXES = ("gx", "gy", "gz")
MESH_ID = pl.DeviceIdType.MESH

RIM = CY - 1
LOW = RIM + 1
HIGH = RIM + 2
SIDE = RIM + 3
INNER = SIDE + CX - 1
TILES = INNER + ((CX - 1) * (CY - 1) + 1) // 2
WIDE = 2 * CZ
BOUND = 2 * INNER
ROWS = BOUND + (CX - 1) * (CY - 1)
AHEAD = 3
SHARE = 6

angle_cosine = -0.6427876096865393
angle_sine = 0.766044443118978


def axis_rows():
    counter = np.arange(NAX) + 0.5
    height = 1.0 - 2.0 * counter / NAX
    radius = np.sqrt(np.maximum(1.0 - height * height, 0.0))
    turning = counter * 2.399963229728653
    rows = np.zeros((8, 128), np.float32)
    rows[0, :NAX] = radius * np.cos(turning)
    rows[1, :NAX] = radius * np.sin(turning)
    rows[2, :NAX] = height
    return rows


def rotate_about(direction, relative):
    inner_product = (
        direction[0] * relative[0] + direction[1] * relative[1] + direction[2] * relative[2]
    )
    crossed = [
        direction[1] * relative[2] - direction[2] * relative[1],
        direction[2] * relative[0] - direction[0] * relative[2],
        direction[0] * relative[1] - direction[1] * relative[0],
    ]
    return [
        relative[component] * angle_cosine
        + crossed[component] * angle_sine
        + direction[component] * inner_product * (1.0 - angle_cosine)
        for component in range(3)
    ]


def take_lanes(values, index):
    return jnp.take_along_axis(values, index, axis=1, mode="promise_in_bounds")


def row_of_plane(ex, ey):
    static = isinstance(ex, int)
    where = (lambda c, a, b: a if c else b) if static else jnp.where
    inner = 2 * INNER + (ex - 1) * (CY - 1) + ey - 1
    last_x = ex == CX
    last_y = ey == CY
    half_x = where(last_x, 1, 0)
    half_y = where(last_y, 1, 0)
    corner = 2 * (LOW + half_y) + half_x
    side_x = 2 * (ey - 1) + half_x
    side_y = 2 * (SIDE + ex - 1) + half_y
    edge_x = (ex == 0) | last_x
    edge_y = (ey == 0) | last_y
    return where(
        edge_x, where(edge_y, corner, side_x), where(edge_y, side_y, inner)
    )


def position_codes(cell):
    plane = (cell * 8129) >> 20
    depth = cell - plane * (CZ + 1)
    ex = (plane * 57) >> 9
    ey = plane - ex * EY
    main = row_of_plane(ex, ey) * 128 + depth
    rim = 2 * RIM * 128 + plane
    return jnp.where(depth == CZ, rim, jnp.where(depth == 0, rim + 128, main))


def neighbours(sizes):
    steps = [(0, 1) if size == 2 else (0, 1, -1) for size in sizes]
    return [
        (dx, dy, dz)
        for dx in steps[0]
        for dy in steps[1]
        for dz in steps[2]
        if (dx, dy, dz) != (0, 0, 0)
    ]


def halo_tiles(step):
    if step[2] != 0:
        return RIM, LOW
    if step[0] != 0:
        return (RIM, SIDE) if step[1] != 0 else (0, SIDE)
    return RIM, INNER


def exchange_kernel(
    sizes,
    slots,
    room,
    shift_hbm,
    target_hbm,
    velocity_hbm,
    cell_hbm,
    rotation_hbm,
    axis_hbm,
    base_ref,
    code_ref,
    table_ref,
    pull_ref,
    shift_ref,
    target_ref,
    velocity_ref,
    cell_ref,
    rotation_ref,
    axis_ref,
    recv_ref,
    send_ref,
    total_ref,
    tile_ref,
    halo_ref,
    block_ref,
    plane_ref,
    kind_ref,
    direction_ref,
    held_ref,
    load_sem,
    send_sem,
    recv_sem,
    halo_send_sem,
    halo_recv_sem,
    near_sem,
    far_sem,
):
    nx, ny, nz = sizes
    devices = nx * ny * nz
    blocks = velocity_ref.shape[1]
    per = 4 * room
    place = tuple(lax.axis_index(axis) for axis in AXES)
    me = (place[0] * ny + place[1]) * nz + place[2]

    loads = [
        pltpu.make_async_copy(source, sink, load_sem.at[i])
        for i, (source, sink) in enumerate(
            (
                (target_hbm, target_ref),
                (cell_hbm, cell_ref),
                (velocity_hbm, velocity_ref),
                (shift_hbm, shift_ref),
                (rotation_hbm, rotation_ref),
                (axis_hbm, axis_ref),
            )
        )
    ]
    for load in loads[:3]:
        load.start()

    def wrap(value, size):
        return jnp.where(value >= size, value - size, value)

    plane = nx * nz
    in_line = ny == 4
    inner_plane = (place[1] == 1) | (place[1] == 2)
    if in_line:
        buddy = jnp.where(place[1] % 2 == 0, place[1] + 1, place[1] - 1)
        upper_half = place[1] >= 2
        across = [jnp.where(upper_half, 1, 2), jnp.where(upper_half, 0, 3)]

    def number_of(there):
        return (there[0] * ny + there[1]) * nz + there[2]

    def partner(k, sign):
        stage, ox, oz = k // plane, k // nz % nx, k % nz
        if sign < 0:
            ox, oz = nx - ox, nz - oz
        if in_line:
            rows = [place[1], buddy, *across]
            if isinstance(stage, int):
                row = rows[stage]
            else:
                row = jnp.where(
                    stage < 2,
                    jnp.where(stage < 1, rows[0], rows[1]),
                    jnp.where(stage < 3, rows[2], rows[3]),
                )
        else:
            row = wrap(place[1] + (ny - stage if sign < 0 else stage), ny)
        return wrap(place[0] + ox, nx), row, wrap(place[2] + oz, nz)

    barrier = pltpu.get_barrier_semaphore()

    def greet(steps):
        for k in steps:
            pl.semaphore_signal(
                barrier, inc=1, device_id=partner(k, 1), device_id_type=MESH_ID
            )

    if in_line:
        greet(range(1, 2 * plane))

        @pl.when(inner_plane)
        def greet_across():
            greet(range(2 * plane, 3 * plane))

    else:
        greet(range(1, devices))

    for load in loads[:3]:
        load.wait()
    for load in loads[3:]:
        load.start()
    target = target_ref[...]
    named = (lax.broadcasted_iota(jnp.int32, (devices, blocks), 0) == target).astype(jnp.float32)
    earlier = (
        lax.broadcasted_iota(jnp.int32, (blocks, blocks), 0)
        < lax.broadcasted_iota(jnp.int32, (blocks, blocks), 1)
    ).astype(jnp.float32)
    before = jnp.dot(
        named.astype(jnp.bfloat16), earlier.astype(jnp.bfloat16), preferred_element_type=jnp.float32
    )
    rank = jnp.sum(named * before, axis=0, keepdims=True).astype(jnp.int32)
    slot = target * room + rank
    chosen = (
        (lax.broadcasted_iota(jnp.int32, (devices * room, blocks), 0) == slot)
        .astype(jnp.float32)
        .astype(jnp.bfloat16)
    )
    codes = position_codes(cell_ref[...]).astype(jnp.float32)
    lanes = codes.shape[1]
    for channel, pair in ((2, (1, 2)), (0, (None, 0))):
        left = jnp.concatenate([codes if c is None else velocity_ref[c] for c in pair], axis=1)
        placed = None
        for part in range(3):
            upper = left.astype(jnp.bfloat16)
            moved = jnp.dot(chosen, upper, preferred_element_type=jnp.float32)
            placed = moved if placed is None else placed + moved
            left = left - upper.astype(jnp.float32)
        send_ref[pl.ds(channel, devices * room, stride=4), :] = placed[:, :lanes]
        send_ref[pl.ds(channel + 1, devices * room, stride=4), :] = placed[:, lanes:]

    def outgoing(k):
        there = partner(k, 1)
        number = number_of(there)
        return pltpu.make_async_remote_copy(
            src_ref=send_ref.at[pl.ds(pl.multiple_of(number * per, 8), per), :],
            dst_ref=recv_ref.at[pl.ds(pl.multiple_of(me * per, 8), per), :],
            send_sem=send_sem.at[number],
            recv_sem=recv_sem.at[me],
            device_id=there,
            device_id_type=MESH_ID,
        )

    def start(steps):
        for k in steps:
            outgoing(k).start()

    if in_line:
        pl.semaphore_wait(barrier, 2 * plane - 1 + jnp.where(inner_plane, plane, 0))

        def tell(semaphore, row):
            there = (place[0], row, place[2])
            pl.semaphore_signal(semaphore, inc=1, device_id=there, device_id_type=MESH_ID)

        @pl.when(inner_plane)
        def pass_on():
            tell(near_sem, across[0])
            tell(near_sem, buddy)

        @pl.when(jnp.logical_not(inner_plane))
        def outer_hears():
            pl.semaphore_wait(near_sem, 1)

        start(range(2 * plane, 2 * plane + AHEAD))

        @pl.when(inner_plane)
        def inner_hears():
            pl.semaphore_wait(near_sem, 1)
            tell(far_sem, buddy)

        @pl.when(jnp.logical_not(inner_plane))
        def outer_hears_again():
            pl.semaphore_wait(far_sem, 1)

        start(range(3 * plane, 3 * plane + AHEAD))
        start(range(1, 2 * plane))
    else:
        pl.semaphore_wait(barrier, devices - 1)
        start(range(1, devices))

    for load in loads[3:]:
        load.wait()
    lane = lax.broadcasted_iota(jnp.int32, (APER, 128), 1)
    depth_index = (lane + place[2] * CZ + shift_ref[2]) % APER
    for ex in range(CX + 1):
        index_x = ((place[0] * CX + ex) % (CX * nx) + shift_ref[0]) % APER
        layer = rotation_ref[index_x].astype(jnp.float32)
        layer = jnp.concatenate([layer] * (128 // APER), axis=1)
        block_ref[ex * APER : (ex + 1) * APER, :] = take_lanes(layer, depth_index)
        for ey in range(EY):
            index_y = ((place[1] * CY + ey) % (CY * ny) + shift_ref[1]) % APER
            row = block_ref[pl.ds(ex * APER + index_y, 1), :]
            plane_ref[ex * EY + ey : ex * EY + ey + 1, :] = row
            at = row_of_plane(ex, ey)
            kind_ref[at : at + 1, :] = row
    planes = plane_ref[0 : 8 * (PLANES // 8 + 1), :]
    sublane = lax.broadcasted_iota(jnp.int32, planes.shape, 0)
    lanes = lax.broadcasted_iota(jnp.int32, planes.shape, 1)
    first = take_lanes(planes, jnp.zeros(planes.shape, jnp.int32))
    rim_kind = jnp.sum(
        jnp.where((sublane == lanes) & (sublane < PLANES), first, 0.0), axis=0, keepdims=True
    )
    kind_ref[2 * RIM : 2 * RIM + 1, :] = rim_kind
    kind_ref[2 * RIM + 1 : 2 * RIM + 2, :] = rim_kind
    kind_ref[ROWS : 2 * TILES, :] = jnp.zeros((2 * TILES - ROWS, 128), jnp.float32)
    kinds = kind_ref[...].astype(jnp.int32)
    for component in range(3):
        direction_ref[component] = take_lanes(
            jnp.broadcast_to(axis_ref[component : component + 1, :], kinds.shape), kinds
        )

    own = pl.ds(pl.multiple_of(me * per, 8), per)
    recv_ref[own, :] = send_ref[own, :]
    total_ref[...] = jnp.zeros(total_ref.shape, jnp.float32)
    pull_ref[...] = jnp.zeros(pull_ref.shape, jnp.float32)
    half = lax.broadcasted_iota(jnp.int32, (8, 128), 0)

    def select_rows(source, rows, row, lane, channels, start):
        found = [jnp.zeros(row.shape, jnp.float32) for c in range(channels)]
        for r in rows:
            here = row == r
            for c in range(channels):
                at = start(r, c)
                line = jnp.broadcast_to(source[at : at + 1, :], row.shape)
                found[c] = jnp.where(here, take_lanes(line, lane), found[c])
        return found

    firsts = [0] if room <= 8 else [*range(0, room - 7, 8)] + ([room - 8] if room % 8 else [])

    def add_sender(k, part):
        base = pl.multiple_of(number_of(partner(k, -1)) * per, 8)
        by_row = lax.broadcasted_iota(jnp.int32, (8 * TILES, 128), 0) >> 3
        by_column = lax.broadcasted_iota(jnp.int32, (WIDE, 128), 0)
        lefts, rights = [], []
        for pair in range(room // 2):
            data = recv_ref[pl.ds(base + 8 * pair, 8), :]
            upper = data.astype(jnp.bfloat16).astype(jnp.float32)
            lower = data - upper
            whole = data.astype(jnp.int32)
            for which in range(2):
                if which == 0:
                    values = jnp.where(half < 4, upper, pltpu.roll(lower, 4, 0))
                else:
                    values = jnp.where(half < 4, pltpu.roll(upper, 4, 0), lower)
                values = jnp.where(half == 0, 1.0, jnp.where(half == 4, 0.0, values))
                code = whole[4 * which : 4 * which + 1]
                tiled = jnp.concatenate([values] * TILES, axis=0)
                lefts.append(jnp.where(by_row == code >> 8, tiled, 0.0).astype(jnp.bfloat16))
                rights.append(
                    (by_column == (code & (WIDE - 1))).astype(jnp.float32).astype(jnp.bfloat16)
                )
        total_ref[part] += lax.dot_general(
            jnp.concatenate(lefts, axis=1),
            jnp.concatenate(rights, axis=1),
            (((1,), (1,)), ((), ())),
            preferred_element_type=jnp.float32,
        )

    def turn_sender(k):
        number = number_of(partner(k, -1))
        base = pl.multiple_of(number * per, 8)

        for first in firsts:
            take = min(8, room)

            def rows_of(channel):
                rows = recv_ref[pl.ds(base + 4 * first + channel, take, stride=4), :]
                return jnp.concatenate([rows] * (8 // take), axis=0)

            code = rows_of(0).astype(jnp.int32)
            kind = select_rows(kind_ref, range(ROWS), code >> 7, code & 127, 1, lambda r, c: r)[0]
            kind = kind.astype(jnp.int32)
            direction = [
                take_lanes(jnp.broadcast_to(axis_ref[c : c + 1, :], (8, 128)), kind)
                for c in range(3)
            ]
            turned = rotate_about(direction, [rows_of(c + 1) for c in range(3)])
            code_ref[pl.ds(first * devices + number, take, stride=devices), :] = code[:take]
            for c in range(3):
                at = (3 * first + c) * devices + number
                base_ref[pl.ds(at, take, stride=3 * devices), :] = turned[c][:take]

    def arrived(k):
        number = number_of(partner(k, -1))
        landing = recv_ref.at[pl.ds(pl.multiple_of(number * per, 8), per), :]
        pltpu.make_async_remote_copy(
            src_ref=landing,
            dst_ref=landing,
            send_sem=send_sem.at[number],
            recv_sem=recv_sem.at[number],
            device_id=place,
            device_id_type=MESH_ID,
        ).wait_recv()

    def add_two(i, carry):
        pair = [2 * i, 2 * i + 1]
        if in_line:
            group = i // 2

            @pl.when((i % 2 == 0) & (group + AHEAD < plane))
            def start_more():
                for stage in (2, 3):
                    outgoing(stage * plane + group).wait_send()
                    outgoing(stage * plane + group + AHEAD).start()

            pair = [
                jnp.where(i < plane, near, far)
                for near, far in zip(pair, (plane + i, 2 * plane + i))
            ]

        @pl.when(i > 0)
        def first_arrived():
            arrived(pair[0])

        arrived(pair[1])
        for part in range(2):
            add_sender(pair[part], part)
        for part in range(2):
            turn_sender(pair[part])
        return carry

    lax.fori_loop(0, devices // 2, add_two, 0)

    for tile in range(TILES):
        rows = pl.ds(8 * tile, 8)
        value = total_ref[0, rows, :] + total_ref[1, rows, :]
        value = value + pltpu.roll(value, 4, 0)
        tile_ref[tile] = jnp.where(half < 4, value[:, :CZ], value[:, CZ:])

    steps = neighbours(sizes)

    def slot_of(step):
        return steps.index(
            tuple(abs(d) if size == 2 else d for d, size in zip(step, sizes))
        )

    copies = []
    for step in steps:
        low, high = halo_tiles(step)
        there = tuple(
            wrap(p + d % size, size) if d else p for p, d, size in zip(place, step, sizes)
        )
        landing = slot_of(tuple(-d for d in step))
        copies.append(
            pltpu.make_async_remote_copy(
                src_ref=tile_ref.at[low:high],
                dst_ref=halo_ref.at[landing, 0 : high - low],
                send_sem=halo_send_sem.at[slot_of(step)],
                recv_sem=halo_recv_sem.at[landing],
                device_id=there,
                device_id_type=MESH_ID,
            )
        )
    for copy in copies:
        copy.start()

    def both(low, high):
        return jnp.where(half < 4, low, high)

    def finish(tile, value):
        count = both(
            jnp.broadcast_to(value[0:1], (8, 128)), jnp.broadcast_to(value[4:5], (8, 128))
        )
        table_ref[8 * tile : 8 * tile + 8, :] = value / jnp.maximum(count, 1.0)

    def pulls(low, high):
        mean = [table_ref[pl.ds(4 * low + 1 + c, high - low, stride=4), :] for c in range(3)]
        direction = [direction_ref[c, low:high, :] for c in range(3)]
        turned = rotate_about(direction, mean)
        for c in range(3):
            pull_ref[pl.ds(4 * low + 1 + c, high - low, stride=4), :] = mean[c] - turned[c]

    def got(step, tile):
        low, high = halo_tiles(step)
        return halo_ref[slot_of(step), tile - low]

    def turned(step, tile):
        return pltpu.roll(got(step, tile), 4, 0)

    groups = devices // 8

    def read_by_lanes(s, low, high):
        for g in range(groups):
            at = pl.multiple_of(s * devices, 8) + 8 * g
            code = code_ref[pl.ds(at, 8), :]
            found = select_rows(
                pull_ref, range(low, high), code >> 7, code & 127, 3, lambda r, c: 4 * r + 1 + c
            )
            for c in range(3):
                there = pl.ds(pl.multiple_of((3 * s + c) * devices, 8) + 8 * g, 8)
                base_ref[there, :] = base_ref[there, :] + found[c]

    def read_by_matrix(s, first, count):
        by_row = lax.broadcasted_iota(jnp.int32, (count, 256), 0) + first
        by_column = lax.broadcasted_iota(jnp.int32, (WIDE, 256), 0)
        for g in range(groups):
            at = pl.multiple_of(s * devices, 8) + 8 * g
            code = code_ref[pl.ds(at, 8), :]
            found = [[], [], []]
            for block in range(0, 8, 2):
                label = jnp.concatenate([code[block : block + 1], code[block + 1 : block + 2]], axis=1)
                onehot = (by_column == (label & (WIDE - 1))).astype(jnp.float32).astype(jnp.bfloat16)
                read = jnp.dot(
                    held_ref[0 : 6 * count, :], onehot, preferred_element_type=jnp.float32
                )
                here = by_row == label >> 8
                for c in range(3):
                    value = read[c * count : (c + 1) * count] + read[(c + 3) * count : (c + 4) * count]
                    line = jnp.sum(jnp.where(here, value, 0.0), axis=0, keepdims=True)
                    found[c] += [line[:, :128], line[:, 128:]]
            for c in range(3):
                there = pl.ds(pl.multiple_of((3 * s + c) * devices, 8) + 8 * g, 8)
                base_ref[there, :] = base_ref[there, :] + jnp.concatenate(found[c], axis=0)

    def read_rows(low, high, first, count):
        for c in range(3):
            value = jnp.concatenate(
                [
                    pull_ref[pl.ds(8 * first + 1 + c, count, stride=8), :],
                    pull_ref[pl.ds(8 * first + 5 + c, count, stride=8), :],
                ],
                axis=1,
            )
            upper = value.astype(jnp.bfloat16)
            held_ref[c * count : (c + 1) * count, :] = upper
            held_ref[(c + 3) * count : (c + 4) * count, :] = (
                value - upper.astype(jnp.float32)
            ).astype(jnp.bfloat16)

        def step(i, carry):
            read_by_matrix(SHARE * i, first, count)
            for other in range(1, SHARE):
                read_by_lanes(SHARE * i + other, low, high)
            return carry

        lax.fori_loop(0, slots // SHARE, step, 0)
        for s in range(slots - slots % SHARE, slots):
            read_by_lanes(s, low, high)

    for tile in range(INNER, TILES):
        finish(tile, tile_ref[tile])
    pulls(BOUND, 2 * TILES)
    read_rows(BOUND, ROWS, TILES - 16, 16)
    for step, copy in zip(steps, copies):
        if step[1:] == (0, 0):
            copy.wait()
    for tile in range(RIM):
        finish(
            tile,
            tile_ref[tile] + both(turned((-1, 0, 0), tile), turned((1, 0, 0), tile)),
        )
    pulls(0, 2 * RIM)
    read_rows(0, 2 * RIM, 0, 8)
    for step, copy in zip(steps, copies):
        if step[1:] != (0, 0):
            copy.wait()
    for k in range(1, devices):
        if not (in_line and k >= 2 * plane and k % plane + AHEAD < plane):
            outgoing(k).wait_send()

    lane = lax.broadcasted_iota(jnp.int32, (8, 128), 1)
    plane_x = (lane * 57) >> 9
    plane_y = lane - plane_x * EY

    def rim(dx, dy):
        own_rim = tile_ref[RIM] if (dx, dy) == (0, 0) else got((dx, dy, 0), RIM)
        return own_rim + both(turned((dx, dy, 1), RIM), turned((dx, dy, -1), RIM))

    for tile in range(RIM, INNER):
        value = tile_ref[tile]
        if tile in (LOW, HIGH):
            value = value + both(turned((-1, 0, 0), tile), turned((1, 0, 0), tile))
        if tile in (LOW, HIGH):
            dy, other = (-1, HIGH) if tile == LOW else (1, LOW)
            value = value + got((0, dy, 0), other)
            value = value + both(turned((-1, dy, 0), other), turned((1, dy, 0), other))
        if SIDE <= tile < INNER:
            value = value + both(turned((0, -1, 0), tile), turned((0, 1, 0), tile))
        if tile == RIM:
            value = rim(0, 0)
            for dx in (-1, 0, 1):
                for dy in (-1, 0, 1):
                    if (dx, dy) == (0, 0):
                        continue
                    inside = lane < PLANES
                    if dx != 0:
                        inside = inside & (plane_x == (CX if dx > 0 else 0))
                    if dy != 0:
                        inside = inside & (plane_y == (CY if dy > 0 else 0))
                    moved = pltpu.roll(rim(dx, dy), (dx * CX * EY + dy * CY) % 128, 1)
                    value = value + jnp.where(inside, moved, 0.0)
        finish(tile, value)
    pulls(2 * RIM, BOUND)


def update_kernel(slots, base_ref, code_ref, table_ref, pull_ref, out_ref, flow_ref):
    devices = out_ref.shape[2]
    sublane = lax.broadcasted_iota(jnp.int32, (CY, 128), 0)
    lane = lax.broadcasted_iota(jnp.int32, (CY, 128), 1)
    for component in range(3):
        rim = table_ref[8 * RIM + 5 + component : 8 * RIM + 6 + component, :]
        rim = jnp.broadcast_to(rim, (CY, 128))
        for ex in range(CX):
            rows = []
            for ey in range(CY):
                at = 4 * row_of_plane(ex, ey) + 1 + component
                rows.append(table_ref[at : at + 1, :])
            flow = jnp.concatenate(rows, axis=0)
            edge = take_lanes(rim, sublane + ex * EY)
            flow_ref[component, ex] = jnp.where(lane == 0, edge, flow)

    def outer(s, carry):
        for g in range(devices // 8):
            code = code_ref[pl.ds(pl.multiple_of(s * devices, 8) + 8 * g, 8), :]
            row, depth = code >> 7, code & 127
            found = [jnp.zeros((8, 128), jnp.float32) for c in range(3)]
            for r in range(2 * RIM, BOUND):
                here = row == r
                for c in range(3):
                    at = 4 * r + 1 + c
                    line = jnp.broadcast_to(pull_ref[at : at + 1, :], (8, 128))
                    found[c] = jnp.where(here, take_lanes(line, depth), found[c])
            for c in range(3):
                at = pl.multiple_of((3 * s + c) * devices, 8) + 8 * g
                out_ref[s, c, 8 * g : 8 * g + 8, :] = base_ref[pl.ds(at, 8), :] + found[c]
        return carry

    lax.fori_loop(0, slots, outer, 0)


def shards(velocity, cell_index, block_target, rotation_axis, grid_shift):
    sizes = tuple(lax.axis_size(axis) for axis in AXES)
    devices = sizes[0] * sizes[1] * sizes[2]
    blocks = velocity.shape[0]
    lanes = velocity.shape[2]
    slots = 3 * blocks // (2 * devices)
    room = slots + slots % 2
    count = len(neighbours(sizes))
    vmem = pl.BlockSpec(memory_space=pltpu.VMEM)
    hbm = pl.BlockSpec(memory_space=pltpu.HBM)
    handed = pl.pallas_call(
        functools.partial(exchange_kernel, sizes, slots, room),
        out_shape=[
            pltpu.VMEM((room * 3 * devices, lanes), jnp.float32),
            pltpu.VMEM((room * devices, lanes), jnp.int32),
            pltpu.VMEM((8 * TILES, lanes), jnp.float32),
            pltpu.VMEM((8 * TILES, lanes), jnp.float32),
        ],
        in_specs=[hbm] * 6,
        out_specs=[vmem] * 4,
        scratch_shapes=[
            pltpu.SMEM((3,), jnp.int32),
            pltpu.VMEM((1, blocks), jnp.int32),
            pltpu.VMEM((3, blocks, lanes), jnp.float32),
            pltpu.VMEM((blocks, lanes), jnp.int32),
            pltpu.VMEM((APER, APER, APER), jnp.int32),
            pltpu.VMEM((8, 128), jnp.float32),
            pltpu.VMEM((devices * room * 4, lanes), jnp.float32),
            pltpu.VMEM((devices * room * 4, lanes), jnp.float32),
            pltpu.VMEM((2, 8 * TILES, WIDE), jnp.float32),
            pltpu.VMEM((TILES, 8, lanes), jnp.float32),
            pltpu.VMEM((count, SIDE, 8, lanes), jnp.float32),
            pltpu.VMEM(((CX + 1) * APER, lanes), jnp.float32),
            pltpu.VMEM((8 * (PLANES // 8 + 1), lanes), jnp.float32),
            pltpu.VMEM((2 * TILES, lanes), jnp.float32),
            pltpu.VMEM((3, 2 * TILES, lanes), jnp.float32),
            pltpu.VMEM((6 * 16, WIDE), jnp.bfloat16),
            pltpu.SemaphoreType.DMA((6,)),
            pltpu.SemaphoreType.DMA((devices,)),
            pltpu.SemaphoreType.DMA((devices,)),
            pltpu.SemaphoreType.DMA((count,)),
            pltpu.SemaphoreType.DMA((count,)),
            pltpu.SemaphoreType.REGULAR,
            pltpu.SemaphoreType.REGULAR,
        ],
        compiler_params=pltpu.CompilerParams(collective_id=0, has_side_effects=True),
        cost_estimate=pl.CostEstimate(flops=1 << 33, bytes_accessed=1 << 21, transcendentals=0),
    )(
        grid_shift,
        block_target.reshape(1, blocks),
        jnp.transpose(velocity, (1, 0, 2)),
        cell_index,
        rotation_axis,
        jnp.asarray(axis_rows()),
    )
    updated, flow = pl.pallas_call(
        functools.partial(update_kernel, slots),
        out_shape=[
            jax.ShapeDtypeStruct((slots, 3, devices, lanes), jnp.float32),
            jax.ShapeDtypeStruct((3, CX, CY, CZ), jnp.float32),
        ],
        in_specs=[vmem] * 4,
        out_specs=[vmem, vmem],
        cost_estimate=pl.CostEstimate(flops=1 << 33, bytes_accessed=1 << 21, transcendentals=0),
    )(*[pltpu.with_memory_space_constraint(array, pltpu.VMEM) for array in handed])
    return (jnp.transpose(updated, (2, 0, 1, 3))[None], flow)


def solution(mesh):
    return jax.shard_map(
        shards,
        mesh=mesh,
        in_specs=(
            P(AXES, None, None),
            P(AXES, None),
            P(AXES, None),
            P(),
            P(),
        ),
        out_specs=(P(AXES, None, None, None, None), P(None, "gx", "gy", "gz")),
        check_vma=False,
    )
```
